256 devices in a mesh: rows: 16 (over x, y), batch: 16 (over z, core).
Axes of the slice: x: 4, y: 4, z: 8, core: 2. Of those that a mesh axis runs over, the one named last changes fastest.
Arguments:
- control: bfloat16 [16, 96, 96, 320], P('batch', 'rows'), may hold values from -60 to 60, as said below
- unet_skips: bfloat16 [2, 16, 96, 96, 320], P(None, 'batch', 'rows'), may hold values from -6 to 6
- norm_gains: float32 [2, 2, 320], replicated, may hold values from 0.25 to 1.75
- norm_shifts: float32 [2, 2, 320], replicated, may hold values from -3 to 3
- conv_weights: bfloat16 [2, 2, 3, 960, 320], P(None, None, None, None, 'batch'), may hold values from -0.109375 to 0.109375
- zero_weights: bfloat16 [2, 1, 320, 320], P(None, None, None, 'batch'), may hold values from -0.3125 to 0.3125
Outputs:
- controls: bfloat16 [2, 16, 96, 96, 320], P(None, 'batch', 'rows')
The draws below stay inside these ranges and needn't reach their ends.
Inputs may be any that keep to these rules, and one draw needn't show every extreme that they name: `control`: Real-valued latent features.
All inputs are finite; a program needn't handle non-finite values.
Results may differ from the reference program's by a relative error of at most 0.01.
Values may be sent and summed in bfloat16 or wider, within the bound.
A program may use at most 64 MiB of HBM per device.

```python
import math
import jax
import jax.numpy as jnp
from jax import lax

C = 320
GROUPS = 32
W = 96
BLOCKS = 2
H = 96
BATCH = 16


def draw_control(key, part):
    first_key = jax.random.fold_in(jax.random.fold_in(key, 17), 0)
    second_key = jax.random.fold_in(jax.random.fold_in(key, 17), 1)
    fourth_key = jax.random.fold_in(jax.random.fold_in(key, 17), 3)
    row_pos = jnp.arange(H, dtype=jnp.float32) / max(H - 1, 1)
    channel_scale = jnp.exp(jax.random.uniform(second_key, (C,), jnp.float32, math.log(0.3), math.log(3.0)))
    channel_offset = jax.random.uniform(fourth_key, (C,), jnp.float32, 0.5, 1.5)
    base = jax.random.truncated_normal(first_key, -6.0, 6.0, (BATCH, H, W, C), jnp.float32)
    row_scale = 1.0 + 2.0 * row_pos
    ramp = 0.5 + 2.5 * row_pos
    values = base * row_scale[None, :, None, None] * channel_scale + ramp[None, :, None, None] * channel_offset
    return values.astype(jnp.bfloat16)


def steps_of(key, dims, cuts, low, largest):
    level = 1.0
    for position, blocks in cuts:
        draws = jax.random.uniform(jax.random.fold_in(jax.random.fold_in(key, 6), position), (blocks,), jnp.float32, low / len(cuts), largest / len(cuts))
        level = level * jnp.repeat(jnp.exp(draws), dims[position] // blocks).reshape((-1,) + (1,) * (len(dims) - 1 - position))
    return level


def gaussian(stream_key, dims, width, reach, cuts=(), kind=jnp.bfloat16):
    result = width * jax.random.normal(stream_key, dims, jnp.float32)
    if cuts:
        result = result * steps_of(stream_key, dims, cuts, -0.22, 0.18)
    return jnp.clip(result, -reach, reach).astype(kind)


def setup_inputs(seed: int = 0) -> dict:
    splits = jax.random.split(jax.random.key(seed), 7)
    return {
        "control": draw_control(jax.random.fold_in(splits[6], 71), 0),
        "unet_skips": gaussian(splits[1], (BLOCKS, BATCH, H, W, C), 1.0, 6.0, ((1, 16), (2, 16))),
        "norm_gains": jnp.clip(1.0 + 0.15 * jax.random.normal(splits[2], (BLOCKS, 2, C), jnp.float32), 0.25, 1.75),
        "norm_shifts": gaussian(splits[3], (BLOCKS, 2, C), 0.5, 3.0, (), jnp.float32),
        "conv_weights": gaussian(splits[4], (BLOCKS, 2, 3, 3 * C, C), (9 * C) ** -0.5, 0.109375, ((4, 16),)),
        "zero_weights": gaussian(splits[5], (BLOCKS, 1, C, C), C ** -0.5, 0.3125, ((3, 16),)),
    }


epsilon = 1e-05

def normalize(values, gain_row, shift_row):
    height, across, channels = values.shape
    grouped = values.astype(jnp.float32).reshape(height, across, GROUPS, channels // GROUPS)
    average = lax.optimization_barrier(jnp.mean(grouped, axis=(0, 1, 3), keepdims=True))
    centered = grouped - average
    spread = lax.optimization_barrier(jnp.mean(centered * centered, axis=(0, 1, 3), keepdims=True))
    scaled = (centered * lax.rsqrt(spread + epsilon)).reshape(height, across, channels) * gain_row + shift_row
    return jax.nn.silu(scaled).astype(jnp.bfloat16)

def convolve(values, weight):
    tap_rows = weight.shape[0]
    tap_cols = weight.shape[1] // values.shape[2]
    margin = tap_rows // 2
    height, across = (values.shape[0], values.shape[1])
    padded = jnp.pad(values, ((margin, margin), (margin, margin), (0, 0)))
    summed = jnp.zeros((height, across, weight.shape[2]), jnp.float32)
    for row_tap in range(tap_rows):
        row_band = padded[row_tap:row_tap + height]
        stacked = jnp.concatenate([row_band[:, col_tap:col_tap + across] for col_tap in range(tap_cols)], axis=2)
        summed = summed + jnp.einsum('hwk,kc->hwc', stacked.astype(jnp.float32), weight[row_tap].astype(jnp.float32))
    return summed

def reference(control, unet_skips, norm_gains, norm_shifts, conv_weights, zero_weights):

    def one_sample(inputs):
        hidden, skip_feats = inputs
        results = []
        for layer_index in range(conv_weights.shape[0]):
            normed = normalize(hidden, norm_gains[layer_index, 0], norm_shifts[layer_index, 0])
            first = convolve(normed, conv_weights[layer_index, 0]).astype(jnp.bfloat16)
            normed_two = normalize(first, norm_gains[layer_index, 1], norm_shifts[layer_index, 1])
            second = convolve(normed_two, conv_weights[layer_index, 1])
            hidden = (hidden.astype(jnp.float32) + second).astype(jnp.bfloat16)
            zeroed = convolve(hidden, zero_weights[layer_index])
            results.append((zeroed + skip_feats[layer_index].astype(jnp.float32)).astype(jnp.bfloat16))
        return jnp.stack(results)
    stacked_out = lax.map(one_sample, (control, jnp.moveaxis(unet_skips, 0, 1)))
    return jnp.moveaxis(stacked_out, 0, 1)
```

```python
import jax
import jax.numpy as jnp
from jax import lax
from jax.experimental import pallas as pl
from jax.experimental.pallas import tpu as pltpu
from jax.sharding import PartitionSpec as P

MESH = pl.DeviceIdType.MESH
F32 = jnp.float32
BF16 = jnp.bfloat16
C = 320
GROUP = 10
W = 96
H = 6
SIDE = 4
RANKS = 16
COL = 16
UNIT = 32
LANES = 1024
EPSILON = 1e-05
MEMBERS = float(96 * 96 * GROUP)


def kernel(
    pieces, control, skips, gains, shifts, out,
    weights, stage, field, halo, left, prod, stats, member, zeros, skip_buf, out_buf,
    load_sem, store_sem, s1_send, s1_recv, bulk_send, a_recv, b_recv, d_recv,
    st_send, st_recv, h_send, h_recv,
):
    rank = lax.axis_index("rows")
    col = lax.axis_index("batch")
    x, y = rank // SIDE, rank % SIDE
    z2, core = (col // 2) * 2, col % 2
    partner = (rank, z2 + 1 - core)

    def at_xy(i, j):
        return lax.rem(x + i, SIDE) * SIDE + lax.rem(y + j, SIDE)

    def unit_rows(r, half=None):
        start = (core * RANKS + r) * UNIT
        if half is None:
            return pl.ds(pl.multiple_of(start, UNIT), UNIT)
        return pl.ds(pl.multiple_of(start + half * 16, 16), 16)

    def send(src, dst, ssem, rsem, target):
        pltpu.make_async_remote_copy(
            src_ref=src, dst_ref=dst, send_sem=ssem, recv_sem=rsem,
            device_id=target, device_id_type=MESH,
        ).start()

    def await_bytes(ref, sem):
        pltpu.make_async_copy(ref, ref, sem).wait()

    load_field = pltpu.make_async_copy(control.at[0], field.at[0], load_sem.at[0])
    load_field.start()
    load_skips = pltpu.make_async_copy(skips, skip_buf, load_sem.at[1])
    load_skips.start()

    barrier = pltpu.get_barrier_semaphore()
    for k in range(1, COL):
        pl.semaphore_signal(barrier, inc=1, device_id=(rank, lax.rem(col + k, COL)), device_id_type=MESH)
    for k in range(1, RANKS):
        pl.semaphore_signal(barrier, inc=1, device_id=(lax.rem(rank + k, RANKS), col), device_id_type=MESH)

    size = 384
    row = lax.broadcasted_iota(jnp.int32, (size, size), 0).astype(F32)
    lane = lax.broadcasted_iota(jnp.int32, (size, size), 1).astype(F32)
    same = jnp.floor((row + 0.5) * (1.0 / GROUP)) == jnp.floor((lane + 0.5) * (1.0 / GROUP))
    member[...] = jnp.where(same, 1.0, 0.0).astype(BF16)

    for g in range(2):
        stage[g, col] = pieces[core, g]
    for p in range(4):

        @pl.when(rank == 0)
        def _():
            halo[p, 0] = jnp.zeros((W, C), BF16)

        @pl.when(rank == RANKS - 1)
        def _():
            halo[p, 1] = jnp.zeros((W, C), BF16)

    load_field.wait()

    lane8 = lax.broadcasted_iota(jnp.int32, (8, 128), 1)
    row8 = lax.broadcasted_iota(jnp.int32, (8, 128), 0)

    def pack_stats(s1, s2):
        s1 = jnp.sum(s1, axis=0, keepdims=True)
        s2 = jnp.sum(s2, axis=0, keepdims=True)
        pad = jnp.zeros((1, 64), F32)
        tile = jnp.zeros((8, 128), F32)
        blocks = []
        for s in (s1, s2):
            blocks += [s[:, 0:128], s[:, 128:256], jnp.concatenate([s[:, 256:320], pad], axis=1)]
        for i, b in enumerate(blocks):
            tile = jnp.where(row8 == i, jnp.broadcast_to(b, (8, 128)), tile)
        return tile

    def start_stats(p, s1, s2):
        stats[p, rank] = pack_stats(s1, s2)
        for k in range(1, RANKS):
            send(stats.at[p, rank], stats.at[p, rank], st_send.at[p], st_recv.at[p],
                 (lax.rem(rank + k, RANKS), col))

    def start_halo(p):
        @pl.when(rank < RANKS - 1)
        def _():
            send(field.at[p, H - 1], halo.at[p, 0], h_send.at[p, 0], h_recv.at[p, 0], (rank + 1, col))

        @pl.when(rank > 0)
        def _():
            send(field.at[p, 0], halo.at[p, 1], h_send.at[p, 1], h_recv.at[p, 1], (rank - 1, col))

    def wait_halo(p):
        @pl.when(rank > 0)
        def _():
            await_bytes(halo.at[p, 0], h_recv.at[p, 0])

        @pl.when(rank < RANKS - 1)
        def _():
            await_bytes(halo.at[p, 1], h_recv.at[p, 1])

    def wait_halo_sends(p):
        @pl.when(rank < RANKS - 1)
        def _():
            await_bytes(halo.at[p, 0], h_send.at[p, 0])

        @pl.when(rank > 0)
        def _():
            await_bytes(halo.at[p, 1], h_send.at[p, 1])

    def fold(v):
        return jnp.sum(v.reshape(W // 8, 8, C), axis=0)

    s1 = jnp.zeros((8, C), F32)
    s2 = jnp.zeros((8, C), F32)
    for i in range(H):
        v = field[0, i].astype(F32)
        s1 = s1 + fold(v)
        s2 = s2 + fold(v * v)

    pl.semaphore_wait(barrier, COL + RANKS - 2)

    for g in range(2):
        for k in range(1, COL):
            to = lax.rem(col + k, COL)
            send(pieces.at[lax.rem(to, 2), g], stage.at[g, col], s1_send.at[g], s1_recv.at[g], (rank, to))
        if g == 0:
            start_stats(0, s1, s2)
            start_halo(0)

    lane_u = lax.broadcasted_iota(jnp.int32, (UNIT, 128), 1)

    def assemble(q):
        g, h = q // 2, q % 2
        acc = [jnp.zeros((UNIT, 128), F32) for _ in range(LANES // 128)]
        for b in range(COL):
            piece = stage[g, b].astype(F32)
            for t in range(3):
                base = 60 * h + 20 * t
                first, last = 20 * b, 20 * b + 20
                cuts = sorted({first, last} | {n for n in (128, 256) if first < n < last})
                rolled = {}
                for lo, hi in zip(cuts, cuts[1:]):
                    dest = 256 * t + lo if lo < 256 else 768 + 64 * t + lo - 256
                    shift = (dest - (base + lo - first)) % 128
                    if shift not in rolled:
                        rolled[shift] = pltpu.roll(piece, shift, 1) if shift else piece
                    d, at = dest // 128, dest % 128
                    mask = (lane_u >= at) & (lane_u < at + hi - lo)
                    acc[d] = jnp.where(mask, rolled[shift], acc[d])
        rows = unit_rows(rank)
        for d in range(LANES // 128):
            weights[q, rows, d * 128 : (d + 1) * 128] = acc[d].astype(BF16)

    def unit_at(q, r, half=None):
        return weights.at[q, unit_rows(r, half)]

    def send_own(q):
        own = unit_at(q, rank)
        for d in range(1, SIDE):
            send(own, own, bulk_send.at[q], a_recv.at[q], (at_xy(d, 0), col))
            send(own, own, bulk_send.at[q], a_recv.at[q], (at_xy(0, d), col))
        send(own, own, bulk_send.at[q], d_recv.at[q], partner)

    def relay(q):
        await_bytes(weights.at[q, pl.ds(0, 6 * UNIT)], a_recv.at[q])
        for d in range(1, SIDE):
            top = unit_at(q, at_xy(SIDE - d, 0), 0)
            bottom = unit_at(q, at_xy(0, SIDE - d), 1)
            for e in range(1, SIDE):
                send(top, top, bulk_send.at[q], b_recv.at[q], (at_xy(0, e), col))
                send(bottom, bottom, bulk_send.at[q], b_recv.at[q], (at_xy(e, 0), col))
        for d in range(1, SIDE):
            for r in (at_xy(SIDE - d, 0), at_xy(0, SIDE - d)):
                send(unit_at(q, r), unit_at(q, r), bulk_send.at[q], d_recv.at[q], partner)

    def finish(q):
        await_bytes(weights.at[q, pl.ds(0, 18 * 16)], b_recv.at[q])
        for d in range(1, SIDE):
            for e in range(1, SIDE):
                r = at_xy(d, e)
                send(unit_at(q, r), unit_at(q, r), bulk_send.at[q], d_recv.at[q], partner)

    def wait_round(q):
        await_bytes(weights.at[q, pl.ds(0, RANKS * UNIT)], d_recv.at[q])

    def read_stats(p):
        await_bytes(stats.at[p, pl.ds(0, RANKS - 1)], st_recv.at[p])
        total = jnp.sum(stats[p], axis=0)
        lines = []
        for s in range(2):
            full = jnp.concatenate([total[3 * s + i : 3 * s + i + 1, :] for i in range(3)], axis=1)
            for _ in range(3):
                part = full.astype(BF16).astype(F32)
                lines.append(part)
                full = full - part
        row = lax.broadcasted_iota(jnp.int32, (8, 384), 0)
        parts = jnp.zeros((8, 384), F32)
        for i, line in enumerate(lines):
            parts = jnp.where(row == i, jnp.broadcast_to(line, (8, 384)), parts)
        sums = jnp.dot(parts.astype(BF16), member[...], preferred_element_type=F32)
        mean = (sums[0:1] + sums[1:2] + sums[2:3])[:, :C] * (1.0 / MEMBERS)
        square = (sums[3:4] + sums[4:5] + sums[5:6])[:, :C] * (1.0 / MEMBERS)
        spread = jnp.maximum(square - mean * mean, 0.0)
        scale = gains[p : p + 1, :] * lax.rsqrt(spread + EPSILON)
        offset = shifts[p : p + 1, :] - mean * scale
        return scale * 0.5, offset * 0.5

    def normalize(p, scale, offset):
        tails = [None] * (H + 2)

        def one(i, raw, keep=None):
            v = raw.astype(F32) * scale + offset
            v = v + v * jnp.tanh(v)
            if keep is not None:
                v = jnp.where(keep, v, 0.0)
            main = v[:, :256].astype(BF16)
            tails[i] = v[:, 256:C]
            for r in range(3):
                o = i - r
                if 0 <= o < H:
                    left[o * W : (o + 1) * W, r * 256 : (r + 1) * 256] = main

        for i in range(H):
            one(i + 1, field[p, i])
        wait_halo(p)
        one(0, halo[p, 0], rank > 0)
        one(H + 1, halo[p, 1], rank < RANKS - 1)
        blank = jnp.zeros((W, 64), F32)
        for o in range(H):
            rows = slice(o * W, (o + 1) * W)
            left[rows, 768:896] = jnp.concatenate([tails[o], tails[o + 1]], axis=1).astype(BF16)
            left[rows, 896:1024] = jnp.concatenate([tails[o + 2], blank], axis=1).astype(BF16)

    edge = lax.broadcasted_iota(jnp.int32, (W, 1), 0)

    def shifted(v, t):
        if t == 1:
            return v
        if t == 0:
            return jnp.where(edge == 0, 0.0, pltpu.roll(v, 1, 0))
        return jnp.where(edge == W - 1, 0.0, pltpu.roll(v, W - 1, 0))

    def conv(p):
        for n in range(4):
            cols = slice(n * 256, (n + 1) * 256)
            prod[:, cols] = jnp.dot(left[...], weights[p, :, cols], preferred_element_type=F32)
        s1 = jnp.zeros((8, C), F32)
        s2 = jnp.zeros((8, C), F32)
        for i in range(H):
            rows = slice(i * W, (i + 1) * W)
            main, tail = 0.0, 0.0
            for t in range(3):
                main = main + shifted(prod[rows, t * 256 : (t + 1) * 256], t)
                tail = tail + shifted(prod[rows, 768 + 64 * t : 768 + 64 * (t + 1)], t)
            v = jnp.concatenate([main, tail], axis=1)
            if p % 2 == 1:
                v = field[p - 1, i].astype(F32) + v
            v = v.astype(BF16)
            field[p + 1, i] = v
            v = v.astype(F32)
            s1 = s1 + fold(v)
            s2 = s2 + fold(v * v)
        return s1, s2

    def zero_conv(b):
        for i in range(4):
            for t in range(3):
                k = 96 * i + 32 * t
                if k < C:
                    rows = slice((30 + i % 2) * UNIT, (31 + i % 2) * UNIT)
                    q = 2 * b + i // 2
                    zeros[k : k + 32, 0:256] = weights[q, rows, 256 * t : 256 * t + 256]
                    block = weights[q, rows, 768 + 128 * (t // 2) : 896 + 128 * (t // 2)].astype(F32)
                    tail = block[:, 64 * (t % 2) : 64 * (t % 2) + 64]
                    zeros[k : k + 32, 256:C] = tail.astype(BF16)
        hidden = field[2 * b + 2].reshape(H * W, C)
        got = jnp.dot(hidden, zeros[...], preferred_element_type=F32).reshape(H, W, C)
        out_buf[b] = (got + skip_buf[b, 0].astype(F32)).astype(BF16)
        pltpu.make_async_copy(out_buf.at[b], out.at[b, 0], store_sem.at[b]).start()

    await_bytes(stage.at[0, pl.ds(0, COL - 1)], s1_recv.at[0])
    assemble(0)
    send_own(0)
    assemble(1)
    send_own(1)
    relay(0)
    await_bytes(stage.at[1, pl.ds(0, COL - 1)], s1_recv.at[1])
    assemble(2)
    assemble(3)
    scale, offset = read_stats(0)
    normalize(0, scale, offset)
    finish(0)
    wait_round(0)
    s1, s2 = conv(0)
    for p in range(1, 4):
        start_stats(p, s1, s2)
        start_halo(p)
        if p + 1 < 4:
            send_own(p + 1)
        relay(p)
        if p == 2:
            load_skips.wait()
            zero_conv(0)
        scale, offset = read_stats(p)
        normalize(p, scale, offset)
        finish(p)
        wait_round(p)
        s1, s2 = conv(p)
    zero_conv(1)

    for b in range(2):
        pltpu.make_async_copy(out_buf.at[b], out.at[b, 0], store_sem.at[b]).wait()
        await_bytes(stage.at[b, pl.ds(0, COL - 1)], s1_send.at[b])
    for p in range(4):
        await_bytes(stats.at[p, pl.ds(0, RANKS - 1)], st_send.at[p])
        wait_halo_sends(p)
        await_bytes(weights.at[p, pl.ds(0, 992)], bulk_send.at[p])


def make_pieces(conv_weights, zero_weights):
    rank = lax.axis_index("rows")
    w = conv_weights.reshape(4, 3, 3, C, 20)

    def cut(tap, start):
        return lax.dynamic_slice(w, (0, tap, 0, start, 0), (4, 1, 3, UNIT, 20))[:, 0]

    low = cut(rank // 8, (rank % 8) * UNIT)
    last = jnp.minimum(jnp.maximum(rank - 8, 0), 5)
    high = cut(
        jnp.where(rank < 8, 2, last // 2),
        jnp.where(rank < 8, (rank % 8) * UNIT, 256 + (last % 2) * UNIT),
    )
    z = jnp.pad(zero_weights[:, 0], ((0, 0), (0, 64), (0, 0))).reshape(2, 2, 2, 3, UNIT, 20)
    z = jnp.where(rank == 15, z[:, :, 1], z[:, :, 0]).reshape(4, 3, UNIT, 20)
    high = jnp.where(rank >= 14, z, high)
    both = jnp.stack([low, high]).reshape(2, 2, 2, 3, UNIT, 20)
    both = both.transpose(0, 1, 4, 2, 3, 5).reshape(2, 2, UNIT, 120)
    return jnp.pad(both, ((0, 0), (0, 0), (0, 0), (0, 8)))


def on_device(control, unet_skips, norm_gains, norm_shifts, conv_weights, zero_weights):
    pieces = make_pieces(conv_weights, zero_weights)
    vmem = pl.BlockSpec(memory_space=pltpu.VMEM)
    hbm = pl.BlockSpec(memory_space=pl.ANY)
    dma = pltpu.SemaphoreType.DMA
    return pl.pallas_call(
        kernel,
        out_shape=jax.ShapeDtypeStruct((2, 1, H, W, C), BF16),
        in_specs=[vmem, hbm, hbm, vmem, vmem],
        out_specs=hbm,
        scratch_shapes=[
            pltpu.VMEM((4, LANES, LANES), BF16),
            pltpu.VMEM((2, COL, UNIT, 128), BF16),
            pltpu.VMEM((5, H, W, C), BF16),
            pltpu.VMEM((4, 2, W, C), BF16),
            pltpu.VMEM((H * W, LANES), BF16),
            pltpu.VMEM((H * W, LANES), F32),
            pltpu.VMEM((4, RANKS, 8, 128), F32),
            pltpu.VMEM((384, 384), BF16),
            pltpu.VMEM((C, C), BF16),
            pltpu.VMEM((2, 1, H, W, C), BF16),
            pltpu.VMEM((2, H, W, C), BF16),
            dma((2,)), dma((2,)), dma((2,)), dma((2,)),
            dma((4,)), dma((4,)), dma((4,)), dma((4,)),
            dma((4,)), dma((4,)), dma((4, 2)), dma((4, 2)),
        ],
        compiler_params=pltpu.CompilerParams(
            collective_id=0, has_side_effects=True, vmem_limit_bytes=60 * 1024 * 1024
        ),
    )(pieces, control, unet_skips, norm_gains.reshape(4, C), norm_shifts.reshape(4, C))


def solution(mesh):
    placed = (
        P("batch", "rows", None, None),
        P(None, "batch", "rows", None, None),
        P(),
        P(),
        P(None, None, None, None, "batch"),
        P(None, None, None, "batch"),
    )
    return jax.shard_map(
        on_device,
        mesh=mesh,
        in_specs=placed,
        out_specs=P(None, "batch", "rows", None, None),
        check_vma=False,
    )
```

```python
import jax
import jax.numpy as jnp
from jax import lax
from jax.experimental import pallas as pl
from jax.experimental.pallas import tpu as pltpu
from jax.sharding import PartitionSpec as P

MESH = pl.DeviceIdType.MESH
F32 = jnp.float32
BF16 = jnp.bfloat16
C = 320
GROUP = 10
W = 96
H = 6
SIDE = 4
RANKS = 16
COL = 16
DEPTH = 8
UNIT = 32
LANES = 1024
EPSILON = 1e-05
MEMBERS = float(96 * 96 * GROUP)


def kernel(
    pieces, control, skips, gains, shifts, out,
    weights, stage, field, halo, left, prod, stats, member, zeros, skip_buf, out_buf,
    load_sem, store_sem, s1_send, s1_recv, bulk_send, a_recv, b_recv, d_recv,
    st_send, st_recv, h_send, h_recv,
):
    rank = lax.axis_index("rows")
    col = lax.axis_index("batch")
    x, y = rank // SIDE, rank % SIDE
    z, core = col // 2, col % 2
    partner = (rank, 2 * z + 1 - core)

    flip_x, flip_y = (z + 1) // 2 % 2, z // 2 % 2
    z_x = lax.rem(z + 1 - 2 * (z % 2), DEPTH)
    z_y = lax.rem(z + DEPTH - 1 + 2 * (z % 2), DEPTH)

    def at_xy(i, j):
        return lax.rem(x + i, SIDE) * SIDE + lax.rem(y + j, SIDE)

    next_x = [(at_xy(1, 0), col), (at_xy(3, 0), col), (rank, 2 * z_x + core)]
    next_y = [(at_xy(0, 1), col), (at_xy(0, 3), col), (rank, 2 * z_y + core)]

    def unit_rows(i, j, half=None):
        a, b = lax.rem(x + i, SIDE), lax.rem(y + j, SIDE)
        inner = 4 * ((a // 2 + flip_x) % 2) + 2 * ((b // 2 + flip_y) % 2) + core
        start = (8 * (2 * (a % 2) + b % 2) + inner) * UNIT
        if half is None:
            return pl.ds(pl.multiple_of(start, UNIT), UNIT)
        return pl.ds(pl.multiple_of(start + half * 16, 16), 16)

    def send(src, dst, ssem, rsem, target):
        pltpu.make_async_remote_copy(
            src_ref=src, dst_ref=dst, send_sem=ssem, recv_sem=rsem,
            device_id=target, device_id_type=MESH,
        ).start()

    def await_bytes(ref, sem):
        pltpu.make_async_copy(ref, ref, sem).wait()

    load_field = pltpu.make_async_copy(control.at[0], field.at[0], load_sem.at[0])
    load_field.start()
    load_skips = pltpu.make_async_copy(skips, skip_buf, load_sem.at[1])
    load_skips.start()

    barrier = pltpu.get_barrier_semaphore()
    for k in range(1, COL):
        pl.semaphore_signal(barrier, inc=1, device_id=(rank, lax.rem(col + k, COL)), device_id_type=MESH)
    for k in range(1, RANKS):
        pl.semaphore_signal(barrier, inc=1, device_id=(lax.rem(rank + k, RANKS), col), device_id_type=MESH)

    size = 384
    row = lax.broadcasted_iota(jnp.int32, (size, size), 0).astype(F32)
    lane = lax.broadcasted_iota(jnp.int32, (size, size), 1).astype(F32)
    same = jnp.floor((row + 0.5) * (1.0 / GROUP)) == jnp.floor((lane + 0.5) * (1.0 / GROUP))
    member[...] = jnp.where(same, 1.0, 0.0).astype(BF16)

    def inner_of(other):
        oz = other // 2
        fx, fy = (oz + 1) // 2 % 2, oz // 2 % 2
        return 4 * ((x // 2 + fx) % 2) + 2 * ((y // 2 + fy) % 2) + other % 2

    mine = inner_of(col)
    for q in range(4):
        stage[q, col] = pieces[mine, q]
    for p in range(4):

        @pl.when(rank == 0)
        def _():
            halo[p, 0] = jnp.zeros((W, C), BF16)

        @pl.when(rank == RANKS - 1)
        def _():
            halo[p, 1] = jnp.zeros((W, C), BF16)

    load_field.wait()

    lane8 = lax.broadcasted_iota(jnp.int32, (8, 128), 1)
    row8 = lax.broadcasted_iota(jnp.int32, (8, 128), 0)

    def pack_stats(s1, s2):
        s1 = jnp.sum(s1, axis=0, keepdims=True)
        s2 = jnp.sum(s2, axis=0, keepdims=True)
        pad = jnp.zeros((1, 64), F32)
        tile = jnp.zeros((8, 128), F32)
        blocks = []
        for s in (s1, s2):
            blocks += [s[:, 0:128], s[:, 128:256], jnp.concatenate([s[:, 256:320], pad], axis=1)]
        for i, b in enumerate(blocks):
            tile = jnp.where(row8 == i, jnp.broadcast_to(b, (8, 128)), tile)
        return tile

    def start_stats(p, s1, s2):
        stats[p, rank] = pack_stats(s1, s2)
        for k in range(1, RANKS):
            send(stats.at[p, rank], stats.at[p, rank], st_send.at[p], st_recv.at[p],
                 (lax.rem(rank + k, RANKS), col))

    def start_halo(p):
        @pl.when(rank < RANKS - 1)
        def _():
            send(field.at[p, H - 1], halo.at[p, 0], h_send.at[p, 0], h_recv.at[p, 0], (rank + 1, col))

        @pl.when(rank > 0)
        def _():
            send(field.at[p, 0], halo.at[p, 1], h_send.at[p, 1], h_recv.at[p, 1], (rank - 1, col))

    def wait_halo(p):
        @pl.when(rank > 0)
        def _():
            await_bytes(halo.at[p, 0], h_recv.at[p, 0])

        @pl.when(rank < RANKS - 1)
        def _():
            await_bytes(halo.at[p, 1], h_recv.at[p, 1])

    def wait_halo_sends(p):
        @pl.when(rank < RANKS - 1)
        def _():
            await_bytes(halo.at[p, 0], h_send.at[p, 0])

        @pl.when(rank > 0)
        def _():
            await_bytes(halo.at[p, 1], h_send.at[p, 1])

    def fold(v):
        return jnp.sum(v.reshape(W // 8, 8, C), axis=0)

    s1 = jnp.zeros((8, C), F32)
    s2 = jnp.zeros((8, C), F32)
    for i in range(H):
        v = field[0, i].astype(F32)
        s1 = s1 + fold(v)
        s2 = s2 + fold(v * v)

    with jax.named_scope("barrier_wait"):
        pl.semaphore_wait(barrier, COL + RANKS - 2)

    def send_pieces(q):
        for k in range(1, COL):
            to = lax.rem(col + k, COL)
            send(pieces.at[inner_of(to), q], stage.at[q, col], s1_send.at[q], s1_recv.at[q], (rank, to))

    def wait_pieces(q):
        await_bytes(stage.at[q, pl.ds(0, COL - 1)], s1_recv.at[q])

    send_pieces(0)
    start_stats(0, s1, s2)
    start_halo(0)
    send_pieces(1)

    lane_u = lax.broadcasted_iota(jnp.int32, (16, 128), 1)

    def assemble(q):
        rows = [unit_rows(0, 0, h) for h in range(2)]
        acc = [[jnp.zeros((16, 128), F32) for _ in range(LANES // 128)] for _ in range(2)]
        for b in range(COL):
            piece = stage[q, b].astype(F32)
            for h in range(2):
                for t in range(3):
                    base = 60 * h + 20 * t
                    first, last = 20 * b, 20 * b + 20
                    cuts = sorted({first, last} | {n for n in (128, 256) if first < n < last})
                    rolled = {}
                    for lo, hi in zip(cuts, cuts[1:]):
                        dest = 256 * t + lo if lo < 256 else 768 + 64 * t + lo - 256
                        shift = (dest - (base + lo - first)) % 128
                        if shift not in rolled:
                            rolled[shift] = pltpu.roll(piece, shift, 1) if shift else piece
                        d, at = dest // 128, dest % 128
                        mask = (lane_u >= at) & (lane_u < at + hi - lo)
                        acc[h][d] = jnp.where(mask, rolled[shift], acc[h][d])
        for h in range(2):
            for d in range(LANES // 128):
                weights[q, rows[h], d * 128 : (d + 1) * 128] = acc[h][d].astype(BF16)

    def unit_at(q, i, j, half=None):
        return weights.at[q, unit_rows(i, j, half)]

    def send_own(q):
        own = unit_at(q, 0, 0)
        for to in next_x + next_y:
            send(own, own, bulk_send.at[q], a_recv.at[q], to)
        send(own, own, bulk_send.at[q], d_recv.at[q], partner)

    def relay(q):
        await_bytes(weights.at[q, pl.ds(0, 6 * UNIT)], a_recv.at[q])
        for d in (1, 3, 2):
            top = unit_at(q, 0, d, 0)
            bottom = unit_at(q, d, 0, 1)
            for to in next_x:
                send(top, top, bulk_send.at[q], b_recv.at[q], to)
            for to in next_y:
                send(bottom, bottom, bulk_send.at[q], b_recv.at[q], to)
        for d in range(1, SIDE):
            for unit in (unit_at(q, 0, d), unit_at(q, d, 0)):
                send(unit, unit, bulk_send.at[q], d_recv.at[q], partner)

    def finish(q):
        await_bytes(weights.at[q, pl.ds(0, 18 * 16)], b_recv.at[q])
        for i in range(1, SIDE):
            for j in range(1, SIDE):
                unit = unit_at(q, i, j)
                send(unit, unit, bulk_send.at[q], d_recv.at[q], partner)

    def wait_round(q):
        await_bytes(weights.at[q, pl.ds(0, RANKS * UNIT)], d_recv.at[q])

    def read_stats(p):
        await_bytes(stats.at[p, pl.ds(0, RANKS - 1)], st_recv.at[p])
        total = jnp.sum(stats[p], axis=0)
        lines = []
        for s in range(2):
            full = jnp.concatenate([total[3 * s + i : 3 * s + i + 1, :] for i in range(3)], axis=1)
            for _ in range(3):
                part = full.astype(BF16).astype(F32)
                lines.append(part)
                full = full - part
        row = lax.broadcasted_iota(jnp.int32, (8, 384), 0)
        parts = jnp.zeros((8, 384), F32)
        for i, line in enumerate(lines):
            parts = jnp.where(row == i, jnp.broadcast_to(line, (8, 384)), parts)
        sums = jnp.dot(parts.astype(BF16), member[...], preferred_element_type=F32)
        mean = (sums[0:1] + sums[1:2] + sums[2:3])[:, :C] * (1.0 / MEMBERS)
        square = (sums[3:4] + sums[4:5] + sums[5:6])[:, :C] * (1.0 / MEMBERS)
        spread = jnp.maximum(square - mean * mean, 0.0)
        scale = gains[p // 2, p % 2 : p % 2 + 1, :] * lax.rsqrt(spread + EPSILON)
        offset = shifts[p // 2, p % 2 : p % 2 + 1, :] - mean * scale
        return scale * 0.5, offset * 0.5

    def normalize(p, scale, offset):
        tails = [None] * (H + 2)

        def one(i, raw, keep=None):
            v = raw.astype(F32) * scale + offset
            v = v + v * jnp.tanh(v)
            if keep is not None:
                v = jnp.where(keep, v, 0.0)
            main = v[:, :256].astype(BF16)
            tails[i] = v[:, 256:C]
            for r in range(3):
                o = i - r
                if 0 <= o < H:
                    left[o * W : (o + 1) * W, r * 256 : (r + 1) * 256] = main

        for i in range(H):
            one(i + 1, field[p, i])
        wait_halo(p)
        one(0, halo[p, 0], rank > 0)
        one(H + 1, halo[p, 1], rank < RANKS - 1)
        blank = jnp.zeros((W, 64), F32)
        for o in range(H):
            rows = slice(o * W, (o + 1) * W)
            left[rows, 768:896] = jnp.concatenate([tails[o], tails[o + 1]], axis=1).astype(BF16)
            left[rows, 896:1024] = jnp.concatenate([tails[o + 2], blank], axis=1).astype(BF16)

    edge = lax.broadcasted_iota(jnp.int32, (W, 1), 0)

    def shifted(v, t):
        if t == 1:
            return v
        if t == 0:
            return jnp.where(edge == 0, 0.0, pltpu.roll(v, 1, 0))
        return jnp.where(edge == W - 1, 0.0, pltpu.roll(v, W - 1, 0))

    def conv(p):
        for n in range(4):
            cols = slice(n * 256, (n + 1) * 256)
            prod[:, cols] = jnp.dot(left[...], weights[p, :, cols], preferred_element_type=F32)
        s1 = jnp.zeros((8, C), F32)
        s2 = jnp.zeros((8, C), F32)
        for i in range(H):
            rows = slice(i * W, (i + 1) * W)
            main, tail = 0.0, 0.0
            for t in range(3):
                main = main + shifted(prod[rows, t * 256 : (t + 1) * 256], t)
                tail = tail + shifted(prod[rows, 768 + 64 * t : 768 + 64 * (t + 1)], t)
            v = jnp.concatenate([main, tail], axis=1)
            if p % 2 == 1:
                v = field[p - 1, i].astype(F32) + v
            v = v.astype(BF16)
            field[p + 1, i] = v
            v = v.astype(F32)
            s1 = s1 + fold(v)
            s2 = s2 + fold(v * v)
        return s1, s2

    def zero_conv(b):
        for i in range(4):
            for t in range(3):
                k = 96 * i + 32 * t
                if k < C:
                    rows = slice((30 + i % 2) * UNIT, (31 + i % 2) * UNIT)
                    q = 2 * b + i // 2
                    zeros[k : k + 32, 0:256] = weights[q, rows, 256 * t : 256 * t + 256]
                    block = weights[q, rows, 768 + 128 * (t // 2) : 896 + 128 * (t // 2)].astype(F32)
                    tail = block[:, 64 * (t % 2) : 64 * (t % 2) + 64]
                    zeros[k : k + 32, 256:C] = tail.astype(BF16)
        hidden = field[2 * b + 2].reshape(H * W, C)
        got = jnp.dot(hidden, zeros[...], preferred_element_type=F32).reshape(H, W, C)
        out_buf[b] = (got + skip_buf[b, 0].astype(F32)).astype(BF16)
        pltpu.make_async_copy(out_buf.at[b], out.at[b, 0], store_sem.at[b]).start()

    def scoped(name, f, *args):
        with jax.named_scope(name):
            return f(*args)

    scoped("s1_wait_0", wait_pieces, 0)
    scoped("assemble_0", assemble, 0)
    send_own(0)
    scoped("s1_wait_1", wait_pieces, 1)
    scoped("assemble_1", assemble, 1)
    send_own(1)
    scoped("relay_0", relay, 0)
    send_pieces(2)
    send_pieces(3)
    scale, offset = scoped("stats_0", read_stats, 0)
    scoped("normalize_0", normalize, 0, scale, offset)
    scoped("relay_1", relay, 1)
    scoped("finish_0", finish, 0)
    scoped("wait_round_0", wait_round, 0)
    s1, s2 = scoped("conv_0", conv, 0)
    for p in range(1, 4):
        start_stats(p, s1, s2)
        start_halo(p)
        scoped(f"finish_{p}", finish, p)
        if p < 3:
            scoped(f"s1_wait_{p + 1}", wait_pieces, p + 1)
            scoped(f"assemble_{p + 1}", assemble, p + 1)
            send_own(p + 1)
        if p == 2:
            load_skips.wait()
            scoped("zero_conv_0", zero_conv, 0)
        scale, offset = scoped(f"stats_{p}", read_stats, p)
        scoped(f"normalize_{p}", normalize, p, scale, offset)
        if p < 3:
            scoped(f"relay_{p + 1}", relay, p + 1)
        scoped(f"wait_round_{p}", wait_round, p)
        s1, s2 = scoped(f"conv_{p}", conv, p)
    scoped("zero_conv_1", zero_conv, 1)

    for b in range(2):
        pltpu.make_async_copy(out_buf.at[b], out.at[b, 0], store_sem.at[b]).wait()
    for p in range(4):
        await_bytes(stage.at[p, pl.ds(0, COL - 1)], s1_send.at[p])
        await_bytes(stats.at[p, pl.ds(0, RANKS - 1)], st_send.at[p])
        wait_halo_sends(p)
        await_bytes(weights.at[p, pl.ds(0, 992)], bulk_send.at[p])


def make_pieces(conv_weights, zero_weights):
    rank = lax.axis_index("rows")
    kind = 2 * (rank // SIDE % 2) + rank % 2
    w = conv_weights.reshape(4, 3, 3, C, 20)
    main = lax.dynamic_slice(w, (0, jnp.minimum(kind, 2), 0, 0, 0), (4, 1, 3, 256, 20))
    main = main[:, 0].transpose(0, 2, 1, 3)
    tails = w[:, :, :, 256:].transpose(0, 1, 3, 2, 4).reshape(4, 192, 3, 20)
    z = jnp.pad(zero_weights[:, 0], ((0, 0), (0, 64), (0, 0))).reshape(2, 2, 2, 3, UNIT, 20)
    z = z.transpose(0, 1, 2, 4, 3, 5).reshape(4, 64, 3, 20)
    rest = jnp.concatenate([tails, z], axis=1)
    both = jnp.where(kind == 3, rest, main).reshape(4, 8, 2, 16, 60)
    both = both.transpose(1, 0, 3, 2, 4).reshape(8, 4, 16, 120)
    return jnp.pad(both, ((0, 0), (0, 0), (0, 0), (0, 8)))


def on_device(control, unet_skips, norm_gains, norm_shifts, conv_weights, zero_weights):
    pieces = make_pieces(conv_weights, zero_weights)
    vmem = pl.BlockSpec(memory_space=pltpu.VMEM)
    hbm = pl.BlockSpec(memory_space=pl.ANY)
    dma = pltpu.SemaphoreType.DMA
    return pl.pallas_call(
        kernel,
        out_shape=jax.ShapeDtypeStruct((2, 1, H, W, C), BF16),
        in_specs=[vmem, hbm, hbm, vmem, vmem],
        out_specs=hbm,
        scratch_shapes=[
            pltpu.VMEM((4, LANES, LANES), BF16),
            pltpu.VMEM((4, COL, 16, 128), BF16),
            pltpu.VMEM((5, H, W, C), BF16),
            pltpu.VMEM((4, 2, W, C), BF16),
            pltpu.VMEM((H * W, LANES), BF16),
            pltpu.VMEM((H * W, LANES), F32),
            pltpu.VMEM((4, RANKS, 8, 128), F32),
            pltpu.VMEM((384, 384), BF16),
            pltpu.VMEM((C, C), BF16),
            pltpu.VMEM((2, 1, H, W, C), BF16),
            pltpu.VMEM((2, H, W, C), BF16),
            dma((2,)), dma((2,)), dma((4,)), dma((4,)),
            dma((4,)), dma((4,)), dma((4,)), dma((4,)),
            dma((4,)), dma((4,)), dma((4, 2)), dma((4, 2)),
        ],
        compiler_params=pltpu.CompilerParams(
            collective_id=0, has_side_effects=True, vmem_limit_bytes=60 * 1024 * 1024
        ),
    )(pieces, control, unet_skips, norm_gains, norm_shifts)


def solution(mesh):
    placed = (
        P("batch", "rows", None, None),
        P(None, "batch", "rows", None, None),
        P(),
        P(),
        P(None, None, None, None, "batch"),
        P(None, None, None, "batch"),
    )
    return jax.shard_map(
        on_device,
        mesh=mesh,
        in_specs=placed,
        out_specs=P(None, "batch", "rows", None, None),
        check_vma=False,
    )
```

```python
import jax
import jax.numpy as jnp
from jax import lax
from jax.experimental import pallas as pl
from jax.experimental.pallas import tpu as pltpu
from jax.sharding import PartitionSpec as P

MESH = pl.DeviceIdType.MESH
F32 = jnp.float32
BF16 = jnp.bfloat16
C = 320
GROUP = 10
W = 96
H = 6
SIDE = 4
RANKS = 16
COL = 16
DEPTH = 8
UNIT = 32
LANES = 1024
EVEN = (3, 2, 2, 2)
EPSILON = 1e-05
MEMBERS = float(96 * 96 * GROUP)


def kernel(
    taps, zero_taps, control, skips, gains, shifts, out,
    raw, raw_zero, pieces, weights, stage, field, halo, left, prod, stats, member, zeros, skip_buf,
    load_sem, s1_send, s1_recv, bulk_send, a_recv, b_recv, d_recv,
    st_send, st_recv, h_send, h_recv,
):
    rank = lax.axis_index("rows")
    col = lax.axis_index("batch")
    x, y = rank // SIDE, rank % SIDE
    z, core = col // 2, col % 2
    partner = (rank, 2 * z + 1 - core)

    flip_x, flip_y = (z + 1) // 2 % 2, z // 2 % 2
    z_x = lax.rem(z + 1 - 2 * (z % 2), DEPTH)
    z_y = lax.rem(z + DEPTH - 1 + 2 * (z % 2), DEPTH)

    def at_xy(i, j):
        return lax.rem(x + i, SIDE) * SIDE + lax.rem(y + j, SIDE)

    next_x = [(at_xy(1, 0), col), (at_xy(3, 0), col), (rank, 2 * z_x + core)]
    next_y = [(at_xy(0, 1), col), (at_xy(0, 3), col), (rank, 2 * z_y + core)]

    def unit_rows(i, j, half=None):
        a, b = lax.rem(x + i, SIDE), lax.rem(y + j, SIDE)
        inner = 4 * ((a // 2 + flip_x) % 2) + 2 * ((b // 2 + flip_y) % 2) + core
        start = (8 * (2 * (a % 2) + b % 2) + inner) * UNIT
        if half is None:
            return pl.ds(pl.multiple_of(start, UNIT), UNIT)
        return pl.ds(pl.multiple_of(start + half * 16, 16), 16)

    def send(src, dst, ssem, rsem, target):
        pltpu.make_async_remote_copy(
            src_ref=src, dst_ref=dst, send_sem=ssem, recv_sem=rsem,
            device_id=target, device_id_type=MESH,
        ).start()

    def await_bytes(ref, sem):
        pltpu.make_async_copy(ref, ref, sem).wait()

    load_field = pltpu.make_async_copy(control.at[0], field.at[0], load_sem.at[0])
    load_raw = [pltpu.make_async_copy(taps.at[b], raw.at[b], load_sem.at[2 + b]) for b in range(2)]
    load_zero = pltpu.make_async_copy(zero_taps, raw_zero, load_sem.at[4])
    load_raw[0].start()
    load_zero.start()
    load_field.start()
    load_raw[1].start()
    load_skips = pltpu.make_async_copy(skips, skip_buf, load_sem.at[1])
    load_skips.start()

    barrier = pltpu.get_barrier_semaphore()
    for k in range(1, COL):
        pl.semaphore_signal(barrier, inc=1, device_id=(rank, lax.rem(col + k, COL)), device_id_type=MESH)
    for k in range(1, RANKS):
        pl.semaphore_signal(barrier, inc=1, device_id=(lax.rem(rank + k, RANKS), col), device_id_type=MESH)

    size = 384
    row = lax.broadcasted_iota(jnp.int32, (size, size), 0).astype(F32)
    lane = lax.broadcasted_iota(jnp.int32, (size, size), 1).astype(F32)
    same = jnp.floor((row + 0.5) * (1.0 / GROUP)) == jnp.floor((lane + 0.5) * (1.0 / GROUP))
    member[...] = jnp.where(same, 1.0, 0.0).astype(BF16)

    def inner_of(other):
        oz = other // 2
        fx, fy = (oz + 1) // 2 % 2, oz // 2 % 2
        return 4 * ((x // 2 + fx) % 2) + 2 * ((y // 2 + fy) % 2) + other % 2

    mine = inner_of(col)
    kind = 2 * (x % 2) + y % 2
    lane_u = lax.broadcasted_iota(jnp.int32, (16, 128), 1)

    def cut_pieces(b):
        def put(q, block, parts):
            rows = jnp.concatenate(parts + [jnp.zeros((4, 128), F32)], axis=0)
            turned = jnp.concatenate([rows.T, jnp.zeros((128, 64), F32)], axis=1)
            for k in range(4):
                low, high = turned[32 * k : 32 * k + 16], turned[32 * k + 16 : 32 * k + 32]
                both = jnp.where(lane_u < 60, low, pltpu.roll(high, 60, 1))
                pieces[4 * block + k, q] = both.astype(BF16)

        @pl.when(kind < 3)
        def _():
            both = raw[b, jnp.minimum(kind, 2)].astype(F32)
            for j in range(2):
                v = both[:, j, :]
                for block in range(2):
                    at = 128 * block
                    put(2 * b + j, block, [v[:, C * t + at : C * t + at + 128] for t in range(3)])

        @pl.when(kind == 3)
        def _():
            both = [raw[b, r].astype(F32) for r in range(3)]
            z = jnp.concatenate([raw_zero[0].astype(F32)[:, b, :], jnp.zeros((20, 64), F32)], axis=1)
            for j in range(2):
                tail = [[both[r][:, j, C * t + 256 : C * t + C] for t in range(3)] for r in range(3)]
                put(2 * b + j, 0, [jnp.concatenate([tail[0][t], tail[1][t]], axis=1) for t in range(3)])
                parts = []
                for t in range(3):
                    cuts = [z[:, 96 * (2 * j + e) + 32 * t : 96 * (2 * j + e) + 32 * t + 32] for e in range(2)]
                    parts.append(jnp.concatenate([tail[2][t]] + cuts, axis=1))
                put(2 * b + j, 1, parts)
        for j in range(2):
            stage[2 * b + j, col] = pieces[mine, 2 * b + j]

    load_raw[0].wait()
    load_zero.wait()
    with jax.named_scope("cut_0"):
        cut_pieces(0)
    load_raw[1].wait()
    with jax.named_scope("cut_1"):
        cut_pieces(1)
    for p in range(4):

        @pl.when(rank == 0)
        def _():
            halo[p, 0] = jnp.zeros((W, C), BF16)

        @pl.when(rank == RANKS - 1)
        def _():
            halo[p, 1] = jnp.zeros((W, C), BF16)

    load_field.wait()

    lane8 = lax.broadcasted_iota(jnp.int32, (8, 128), 1)
    row8 = lax.broadcasted_iota(jnp.int32, (8, 128), 0)

    def pack_stats(s1, s2):
        s1 = jnp.sum(s1, axis=0, keepdims=True)
        s2 = jnp.sum(s2, axis=0, keepdims=True)
        pad = jnp.zeros((1, 64), F32)
        tile = jnp.zeros((8, 128), F32)
        blocks = []
        for s in (s1, s2):
            blocks += [s[:, 0:128], s[:, 128:256], jnp.concatenate([s[:, 256:320], pad], axis=1)]
        for i, b in enumerate(blocks):
            tile = jnp.where(row8 == i, jnp.broadcast_to(b, (8, 128)), tile)
        return tile

    def start_stats(p, s1, s2):
        stats[p, rank] = pack_stats(s1, s2)
        for k in range(1, RANKS):
            send(stats.at[p, rank], stats.at[p, rank], st_send.at[p], st_recv.at[p],
                 (lax.rem(rank + k, RANKS), col))

    def start_halo(p):
        @pl.when(rank < RANKS - 1)
        def _():
            send(field.at[p, H - 1], halo.at[p, 0], h_send.at[p, 0], h_recv.at[p, 0], (rank + 1, col))

        @pl.when(rank > 0)
        def _():
            send(field.at[p, 0], halo.at[p, 1], h_send.at[p, 1], h_recv.at[p, 1], (rank - 1, col))

    def wait_halo(p):
        @pl.when(rank > 0)
        def _():
            await_bytes(halo.at[p, 0], h_recv.at[p, 0])

        @pl.when(rank < RANKS - 1)
        def _():
            await_bytes(halo.at[p, 1], h_recv.at[p, 1])

    def wait_halo_sends(p):
        @pl.when(rank < RANKS - 1)
        def _():
            await_bytes(halo.at[p, 0], h_send.at[p, 0])

        @pl.when(rank > 0)
        def _():
            await_bytes(halo.at[p, 1], h_send.at[p, 1])

    def fold(v):
        return jnp.sum(v.reshape(W // 8, 8, C), axis=0)

    s1 = jnp.zeros((8, C), F32)
    s2 = jnp.zeros((8, C), F32)
    for i in range(H):
        v = field[0, i].astype(F32)
        s1 = s1 + fold(v)
        s2 = s2 + fold(v * v)

    with jax.named_scope("barrier_wait"):
        pl.semaphore_wait(barrier, COL + RANKS - 2)

    def send_pieces(q):
        for k in range(1, COL):
            to = lax.rem(col + k, COL)
            send(pieces.at[inner_of(to), q], stage.at[q, col], s1_send.at[q], s1_recv.at[q], (rank, to))

    def wait_pieces(q):
        await_bytes(stage.at[q, pl.ds(0, COL - 1)], s1_recv.at[q])

    send_pieces(0)
    start_stats(0, s1, s2)
    start_halo(0)
    send_pieces(1)

    def assemble(q):
        rows = [unit_rows(0, 0, h) for h in range(2)]
        acc = [[jnp.zeros((16, 128), F32) for _ in range(LANES // 128)] for _ in range(2)]
        for b in range(COL):
            piece = stage[q, b].astype(F32)
            for h in range(2):
                for t in range(3):
                    base = 60 * h + 20 * t
                    first, last = 20 * b, 20 * b + 20
                    cuts = sorted({first, last} | {n for n in (128, 256) if first < n < last})
                    rolled = {}
                    for lo, hi in zip(cuts, cuts[1:]):
                        dest = 256 * t + lo if lo < 256 else 768 + 64 * t + lo - 256
                        shift = (dest - (base + lo - first)) % 128
                        if shift not in rolled:
                            rolled[shift] = pltpu.roll(piece, shift, 1) if shift else piece
                        d, at = dest // 128, dest % 128
                        mask = (lane_u >= at) & (lane_u < at + hi - lo)
                        acc[h][d] = jnp.where(mask, rolled[shift], acc[h][d])
        for h in range(2):
            for d in range(LANES // 128):
                weights[q, rows[h], d * 128 : (d + 1) * 128] = acc[h][d].astype(BF16)

    def unit_at(q, i, j, half=None):
        return weights.at[q, unit_rows(i, j, half)]

    def send_own(q):
        own = unit_at(q, 0, 0)
        for to in next_x + next_y:
            send(own, own, bulk_send.at[q], a_recv.at[q], to)
        send(own, own, bulk_send.at[q], d_recv.at[q], partner)

    def relay(q):
        await_bytes(weights.at[q, pl.ds(0, 6 * UNIT)], a_recv.at[q])

        def forward(unit, targets):
            for to in targets:
                send(unit, unit, bulk_send.at[q], b_recv.at[q], to)

        for d in (1, 3):
            forward(unit_at(q, 0, d, 0), next_x[: EVEN[q]])
            forward(unit_at(q, d, 0, 1), next_y[: EVEN[q]])
        forward(unit_at(q, 0, 2, 0), next_x)
        forward(unit_at(q, 2, 0, 1), next_y)
        if EVEN[q] == 2:
            forward(unit_at(q, 0, 2, 1), next_x[:2])
            forward(unit_at(q, 2, 0, 0), next_y[:2])
        for d in range(1, SIDE):
            for unit in (unit_at(q, 0, d), unit_at(q, d, 0)):
                send(unit, unit, bulk_send.at[q], d_recv.at[q], partner)

    def finish(q):
        await_bytes(weights.at[q, pl.ds(0, 18 * 16)], b_recv.at[q])
        for i in range(1, SIDE):
            for j in range(1, SIDE):
                unit = unit_at(q, i, j)
                send(unit, unit, bulk_send.at[q], d_recv.at[q], partner)

    def wait_round(q):
        await_bytes(weights.at[q, pl.ds(0, RANKS * UNIT)], d_recv.at[q])

    def read_stats(p):
        await_bytes(stats.at[p, pl.ds(0, RANKS - 1)], st_recv.at[p])
        total = jnp.sum(stats[p], axis=0)
        lines = []
        for s in range(2):
            full = jnp.concatenate([total[3 * s + i : 3 * s + i + 1, :] for i in range(3)], axis=1)
            for _ in range(3):
                part = full.astype(BF16).astype(F32)
                lines.append(part)
                full = full - part
        row = lax.broadcasted_iota(jnp.int32, (8, 384), 0)
        parts = jnp.zeros((8, 384), F32)
        for i, line in enumerate(lines):
            parts = jnp.where(row == i, jnp.broadcast_to(line, (8, 384)), parts)
        sums = jnp.dot(parts.astype(BF16), member[...], preferred_element_type=F32)
        mean = (sums[0:1] + sums[1:2] + sums[2:3])[:, :C] * (1.0 / MEMBERS)
        square = (sums[3:4] + sums[4:5] + sums[5:6])[:, :C] * (1.0 / MEMBERS)
        spread = jnp.maximum(square - mean * mean, 0.0)
        scale = gains[p // 2, p % 2 : p % 2 + 1, :] * lax.rsqrt(spread + EPSILON)
        offset = shifts[p // 2, p % 2 : p % 2 + 1, :] - mean * scale
        return scale * 0.5, offset * 0.5

    def normalize(p, scale, offset):
        tails = [None] * (H + 2)

        def one(i, raw, keep=None):
            v = raw.astype(F32) * scale + offset
            v = v + v * jnp.tanh(v)
            if keep is not None:
                v = jnp.where(keep, v, 0.0)
            main = v[:, :256].astype(BF16)
            tails[i] = v[:, 256:C]
            for r in range(3):
                o = i - r
                if 0 <= o < H:
                    left[o * W : (o + 1) * W, r * 256 : (r + 1) * 256] = main

        for i in range(H):
            one(i + 1, field[p, i])
        wait_halo(p)
        one(0, halo[p, 0], rank > 0)
        one(H + 1, halo[p, 1], rank < RANKS - 1)
        blank = jnp.zeros((W, 64), F32)
        for o in range(H):
            rows = slice(o * W, (o + 1) * W)
            left[rows, 768:896] = jnp.concatenate([tails[o], tails[o + 1]], axis=1).astype(BF16)
            left[rows, 896:1024] = jnp.concatenate([tails[o + 2], blank], axis=1).astype(BF16)

    edge = lax.broadcasted_iota(jnp.int32, (W, 1), 0)

    def shifted(v, t):
        if t == 1:
            return v
        if t == 0:
            return jnp.where(edge == 0, 0.0, pltpu.roll(v, 1, 0))
        return jnp.where(edge == W - 1, 0.0, pltpu.roll(v, W - 1, 0))

    def conv(p):
        for n in range(4):
            cols = slice(n * 256, (n + 1) * 256)
            prod[:, cols] = jnp.dot(left[...], weights[p, :, cols], preferred_element_type=F32)
        s1 = jnp.zeros((8, C), F32)
        s2 = jnp.zeros((8, C), F32)
        for i in range(H):
            rows = slice(i * W, (i + 1) * W)
            main, tail = 0.0, 0.0
            for t in range(3):
                main = main + shifted(prod[rows, t * 256 : (t + 1) * 256], t)
                tail = tail + shifted(prod[rows, 768 + 64 * t : 768 + 64 * (t + 1)], t)
            v = jnp.concatenate([main, tail], axis=1)
            if p % 2 == 1:
                v = field[p - 1, i].astype(F32) + v
            v = v.astype(BF16)
            field[p + 1, i] = v
            v = v.astype(F32)
            s1 = s1 + fold(v)
            s2 = s2 + fold(v * v)
        return s1, s2

    def zero_conv(b):
        for i in range(4):
            for t in range(3):
                k = 96 * i + 32 * t
                if k < C:
                    rows = slice((30 + i % 2) * UNIT, (31 + i % 2) * UNIT)
                    q = 2 * b + i // 2
                    zeros[k : k + 32, 0:256] = weights[q, rows, 256 * t : 256 * t + 256]
                    block = weights[q, rows, 768 + 128 * (t // 2) : 896 + 128 * (t // 2)].astype(F32)
                    tail = block[:, 64 * (t % 2) : 64 * (t % 2) + 64]
                    zeros[k : k + 32, 256:C] = tail.astype(BF16)
        hidden = field[2 * b + 2].reshape(H * W, C)
        got = jnp.dot(hidden, zeros[...], preferred_element_type=F32).reshape(H, W, C)
        out[b, 0] = (got + skip_buf[b, 0].astype(F32)).astype(BF16)

    def scoped(name, f, *args):
        with jax.named_scope(name):
            return f(*args)

    scoped("s1_wait_0", wait_pieces, 0)
    scoped("assemble_0", assemble, 0)
    send_own(0)
    scoped("s1_wait_1", wait_pieces, 1)
    scoped("assemble_1", assemble, 1)
    send_own(1)
    scoped("relay_0", relay, 0)
    send_pieces(2)
    scale, offset = scoped("stats_0", read_stats, 0)
    scoped("normalize_0", normalize, 0, scale, offset)
    scoped("finish_0", finish, 0)
    scoped("relay_1", relay, 1)
    send_pieces(3)
    scoped("s1_wait_2", wait_pieces, 2)
    scoped("assemble_2", assemble, 2)
    scoped("wait_round_0", wait_round, 0)
    send_own(2)
    s1, s2 = scoped("conv_0", conv, 0)
    for p in range(1, 4):
        start_stats(p, s1, s2)
        start_halo(p)
        scoped(f"finish_{p}", finish, p)
        if p == 1:
            scoped("s1_wait_3", wait_pieces, 3)
            scoped("assemble_3", assemble, 3)
        if p < 3:
            scoped(f"relay_{p + 1}", relay, p + 1)
        if p == 1:
            send_own(3)
        if p == 2:
            load_skips.wait()
            scoped("zero_conv_0", zero_conv, 0)
        scale, offset = scoped(f"stats_{p}", read_stats, p)
        scoped(f"normalize_{p}", normalize, p, scale, offset)
        scoped(f"wait_round_{p}", wait_round, p)
        s1, s2 = scoped(f"conv_{p}", conv, p)
    scoped("zero_conv_1", zero_conv, 1)

    for p in range(4):
        await_bytes(stage.at[p, pl.ds(0, COL - 1)], s1_send.at[p])
        await_bytes(stats.at[p, pl.ds(0, RANKS - 1)], st_send.at[p])
        wait_halo_sends(p)
        await_bytes(weights.at[p, pl.ds(0, 992)], bulk_send.at[p])


def on_device(control, unet_skips, norm_gains, norm_shifts, conv_weights, zero_weights):
    vmem = pl.BlockSpec(memory_space=pltpu.VMEM)
    hbm = pl.BlockSpec(memory_space=pl.ANY)
    dma = pltpu.SemaphoreType.DMA
    return pl.pallas_call(
        kernel,
        out_shape=pltpu.VMEM((2, 1, H, W, C), BF16),
        in_specs=[hbm, hbm, hbm, hbm, vmem, vmem],
        out_specs=vmem,
        scratch_shapes=[
            pltpu.VMEM((2, 3, 20, 2, 3 * C), BF16),
            pltpu.VMEM((1, 20, 2, C), BF16),
            pltpu.VMEM((8, 4, 16, 128), BF16),
            pltpu.VMEM((4, LANES, LANES), BF16),
            pltpu.VMEM((4, COL, 16, 128), BF16),
            pltpu.VMEM((5, H, W, C), BF16),
            pltpu.VMEM((4, 2, W, C), BF16),
            pltpu.VMEM((H * W, LANES), BF16),
            pltpu.VMEM((H * W, LANES), F32),
            pltpu.VMEM((4, RANKS, 8, 128), F32),
            pltpu.VMEM((384, 384), BF16),
            pltpu.VMEM((C, C), BF16),
            pltpu.VMEM((2, 1, H, W, C), BF16),
            dma((5,)), dma((4,)), dma((4,)),
            dma((4,)), dma((4,)), dma((4,)), dma((4,)),
            dma((4,)), dma((4,)), dma((4, 2)), dma((4, 2)),
        ],
        compiler_params=pltpu.CompilerParams(
            collective_id=0, has_side_effects=True, vmem_limit_bytes=66_150_400
        ),
    )(
        conv_weights.transpose(0, 2, 4, 1, 3), zero_weights.transpose(1, 3, 0, 2),
        control, unet_skips, norm_gains, norm_shifts,
    )


def solution(mesh):
    placed = (
        P("batch", "rows", None, None),
        P(None, "batch", "rows", None, None),
        P(),
        P(),
        P(None, None, None, None, "batch"),
        P(None, None, None, "batch"),
    )
    return jax.shard_map(
        on_device,
        mesh=mesh,
        in_specs=placed,
        out_specs=P(None, "batch", "rows", None, None),
        check_vma=False,
    )
```

```python
import jax
import jax.numpy as jnp
from jax import lax
from jax.experimental import pallas as pl
from jax.experimental.pallas import tpu as pltpu
from jax.sharding import PartitionSpec as P

MESH = pl.DeviceIdType.MESH
F32 = jnp.float32
BF16 = jnp.bfloat16
C = 320
GROUP = 10
W = 96
H = 6
SIDE = 4
RANKS = 16
COL = 16
DEPTH = 8
UNIT = 32
LANES = 1024
EVEN = (3, 2, 3, 3)
STEPS = (1, 3, 2)
PART = 3
FAR_FIRST = (
    (2, 2), (1, 2), (3, 2), (2, 1), (2, 3), (1, 1), (1, 3), (3, 1), (3, 3), (0, 2), (2, 0), (0, 1), (0, 3), (1, 0), (3, 0)
)
FAR_COLUMN = (8, 7, 9, 6, 10, 5, 11, 4, 12, 3, 13, 2, 14, 1, 15)
EPSILON = 1e-05
MEMBERS = float(96 * 96 * GROUP)


def kernel(
    taps, zero_taps, control, skips, gain_rows, shift_rows, out,
    raw, raw_zero, pieces, weights, stage, field, halo, left, prod, stats, gather, spread_out, zeros, skip_buf, gains, shifts,
    load_sem, s1_send, s1_recv, bulk_send, a_recv, b_recv, d_recv,
    st_send, st_recv, h_send, h_recv,
):
    rank = lax.axis_index("rows")
    col = lax.axis_index("batch")
    x, y = rank // SIDE, rank % SIDE
    z, core = col // 2, col % 2
    partner = (rank, 2 * z + 1 - core)

    flip_x, flip_y = (z + 1) // 2 % 2, z // 2 % 2
    z_x = lax.rem(z + 1 - 2 * (z % 2), DEPTH)
    z_y = lax.rem(z + DEPTH - 1 + 2 * (z % 2), DEPTH)

    def at_xy(i, j):
        return lax.rem(x + i, SIDE) * SIDE + lax.rem(y + j, SIDE)

    next_x = [(at_xy(1, 0), col), (at_xy(3, 0), col), (rank, 2 * z_x + core)]
    next_y = [(at_xy(0, 1), col), (at_xy(0, 3), col), (rank, 2 * z_y + core)]

    def unit_rows(i, j, half=None):
        a, b = lax.rem(x + i, SIDE), lax.rem(y + j, SIDE)
        inner = 4 * ((a // 2 + flip_x) % 2) + 2 * ((b // 2 + flip_y) % 2) + core
        start = (8 * (2 * (a % 2) + b % 2) + inner) * UNIT
        if half is None:
            return pl.ds(pl.multiple_of(start, UNIT), UNIT)
        return pl.ds(pl.multiple_of(start + half * 16, 16), 16)

    def send(src, dst, ssem, rsem, target):
        pltpu.make_async_remote_copy(
            src_ref=src, dst_ref=dst, send_sem=ssem, recv_sem=rsem,
            device_id=target, device_id_type=MESH,
        ).start()

    def await_bytes(ref, sem):
        pltpu.make_async_copy(ref, ref, sem).wait()

    barrier = pltpu.get_barrier_semaphore()
    for k in range(1, COL):
        pl.semaphore_signal(barrier, inc=1, device_id=(rank, lax.rem(col + k, COL)), device_id_type=MESH)
    for k in range(1, RANKS):
        pl.semaphore_signal(barrier, inc=1, device_id=(lax.rem(rank + k, RANKS), col), device_id_type=MESH)

    load_field = pltpu.make_async_copy(control.at[0], field.at[0], load_sem.at[0])
    load_raw = [pltpu.make_async_copy(taps.at[b], raw.at[b], load_sem.at[2 + b]) for b in range(2)]
    load_zero = pltpu.make_async_copy(zero_taps, raw_zero, load_sem.at[4])
    load_raw[0].start()
    load_zero.start()
    load_field.start()
    load_raw[1].start()
    load_skips = pltpu.make_async_copy(skips, skip_buf, load_sem.at[1])
    load_skips.start()
    load_rows = [
        pltpu.make_async_copy(gain_rows, gains, load_sem.at[5]),
        pltpu.make_async_copy(shift_rows, shifts, load_sem.at[6]),
    ]
    for load in load_rows:
        load.start()

    def belongs(shape, channels, groups):
        channel = lax.broadcasted_iota(jnp.int32, shape, channels).astype(F32)
        group = (lax.broadcasted_iota(jnp.int32, shape, groups) % 64).astype(F32)
        same = jnp.floor((channel + 0.5) * (1.0 / GROUP)) == group
        return jnp.where(same, 1.0, 0.0).astype(BF16)

    gather[...] = belongs((384, 128), 0, 1)
    spread_out[...] = belongs((64, 384), 1, 0)

    def inner_of(other):
        oz = other // 2
        fx, fy = (oz + 1) // 2 % 2, oz // 2 % 2
        return 4 * ((x // 2 + fx) % 2) + 2 * ((y // 2 + fy) % 2) + other % 2

    mine = inner_of(col)
    kind = 2 * (x % 2) + y % 2
    lane_u = lax.broadcasted_iota(jnp.int32, (16, 128), 1)

    def cut_pieces(b):
        def put(q, block, parts):
            rows = jnp.concatenate(parts + [jnp.zeros((4, 128), F32)], axis=0)
            turned = jnp.concatenate([rows.T, jnp.zeros((128, 64), F32)], axis=1)
            for k in range(4):
                low, high = turned[32 * k : 32 * k + 16], turned[32 * k + 16 : 32 * k + 32]
                both = jnp.where(lane_u < 60, low, pltpu.roll(high, 60, 1))
                pieces[4 * block + k, q] = both.astype(BF16)

        @pl.when(kind < 3)
        def _():
            both = raw[b, jnp.minimum(kind, 2)].astype(F32)
            for j in range(2):
                v = both[:, j, :]
                for block in range(2):
                    at = 128 * block
                    put(2 * b + j, block, [v[:, C * t + at : C * t + at + 128] for t in range(3)])

        @pl.when(kind == 3)
        def _():
            both = [raw[b, r].astype(F32) for r in range(3)]
            z = jnp.concatenate([raw_zero[0].astype(F32)[:, b, :], jnp.zeros((20, 64), F32)], axis=1)
            for j in range(2):
                tail = [[both[r][:, j, C * t + 256 : C * t + C] for t in range(3)] for r in range(3)]
                put(2 * b + j, 0, [jnp.concatenate([tail[0][t], tail[1][t]], axis=1) for t in range(3)])
                parts = []
                for t in range(3):
                    cuts = [z[:, 96 * (2 * j + e) + 32 * t : 96 * (2 * j + e) + 32 * t + 32] for e in range(2)]
                    parts.append(jnp.concatenate([tail[2][t]] + cuts, axis=1))
                put(2 * b + j, 1, parts)
        for j in range(2):
            stage[2 * b + j, col] = pieces[mine, 2 * b + j]

    load_raw[0].wait()
    load_zero.wait()
    with jax.named_scope("cut_0"):
        cut_pieces(0)
    load_raw[1].wait()
    with jax.named_scope("cut_1"):
        cut_pieces(1)
    for p in range(4):

        @pl.when(rank == 0)
        def _():
            halo[p, 0] = jnp.zeros((W, C), BF16)

        @pl.when(rank == RANKS - 1)
        def _():
            halo[p, 1] = jnp.zeros((W, C), BF16)

    load_field.wait()

    lane1 = lax.broadcasted_iota(jnp.int32, (1, 128), 1)

    def three_parts(v):
        parts = []
        for _ in range(3):
            part = v.astype(BF16).astype(F32)
            parts.append(part)
            v = v - part
        return parts

    def pack_stats(s1, s2):
        both = jnp.concatenate([jnp.concatenate([s1, s2], axis=0), jnp.zeros((16, 64), F32)], axis=1)
        parts = jnp.concatenate(three_parts(both), axis=0).astype(BF16)
        sums = jnp.dot(parts, gather[...], preferred_element_type=F32)
        sums = sums[0:16] + sums[16:32] + sums[32:48]
        first = jnp.sum(sums[0:8], axis=0, keepdims=True)
        second = jnp.sum(sums[8:16], axis=0, keepdims=True)
        return jnp.where(lane1 < 64, first, second)

    def start_stats(p, s1, s2):
        stats[p, rank] = pack_stats(s1, s2)
        for i, j in FAR_FIRST:
            send(stats.at[p, rank], stats.at[p, rank], st_send.at[p], st_recv.at[p], (at_xy(i, j), col))

    def start_halo(p):
        @pl.when(rank < RANKS - 1)
        def _():
            send(field.at[p, H - 1], halo.at[p, 0], h_send.at[p, 0], h_recv.at[p, 0], (rank + 1, col))

        @pl.when(rank > 0)
        def _():
            send(field.at[p, 0], halo.at[p, 1], h_send.at[p, 1], h_recv.at[p, 1], (rank - 1, col))

    def wait_halo(p):
        @pl.when(rank > 0)
        def _():
            await_bytes(halo.at[p, 0], h_recv.at[p, 0])

        @pl.when(rank < RANKS - 1)
        def _():
            await_bytes(halo.at[p, 1], h_recv.at[p, 1])

    def wait_halo_sends(p):
        @pl.when(rank < RANKS - 1)
        def _():
            await_bytes(halo.at[p, 0], h_send.at[p, 0])

        @pl.when(rank > 0)
        def _():
            await_bytes(halo.at[p, 1], h_send.at[p, 1])

    def fold(v):
        return jnp.sum(v.reshape(W // 8, 8, C), axis=0)

    s1 = jnp.zeros((8, C), F32)
    s2 = jnp.zeros((8, C), F32)
    for i in range(H):
        v = field[0, i].astype(F32)
        s1 = s1 + fold(v)
        s2 = s2 + fold(v * v)

    with jax.named_scope("barrier_wait"):
        pl.semaphore_wait(barrier, COL + RANKS - 2)

    def send_pieces(q):
        for k in FAR_COLUMN:
            to = lax.rem(col + k, COL)
            send(pieces.at[inner_of(to), q], stage.at[q, col], s1_send.at[q], s1_recv.at[q], (rank, to))

    def wait_pieces(q):
        await_bytes(stage.at[q, pl.ds(0, COL - 1)], s1_recv.at[q])

    send_pieces(0)
    start_stats(0, s1, s2)
    start_halo(0)
    send_pieces(1)

    def assemble(q):
        rows = [unit_rows(0, 0, h) for h in range(2)]
        acc = [[jnp.zeros((16, 128), F32) for _ in range(LANES // 128)] for _ in range(2)]
        for b in range(COL):
            piece = stage[q, b].astype(F32)
            for h in range(2):
                for t in range(3):
                    base = 60 * h + 20 * t
                    first, last = 20 * b, 20 * b + 20
                    cuts = sorted({first, last} | {n for n in (128, 256) if first < n < last})
                    rolled = {}
                    for lo, hi in zip(cuts, cuts[1:]):
                        dest = 256 * t + lo if lo < 256 else 768 + 64 * t + lo - 256
                        shift = (dest - (base + lo - first)) % 128
                        if shift not in rolled:
                            rolled[shift] = pltpu.roll(piece, shift, 1) if shift else piece
                        d, at = dest // 128, dest % 128
                        mask = (lane_u >= at) & (lane_u < at + hi - lo)
                        acc[h][d] = jnp.where(mask, rolled[shift], acc[h][d])
        for h in range(2):
            for d in range(LANES // 128):
                weights[q, rows[h], d * 128 : (d + 1) * 128] = acc[h][d].astype(BF16)

    def unit_at(q, i, j, half=None):
        return weights.at[q, unit_rows(i, j, half)]

    def send_own(q):
        own = unit_at(q, 0, 0)
        first, last = unit_at(q, 0, 0, 0), unit_at(q, 0, 0, 1)
        for step in range(2):
            for to_x, to_y in zip(next_x, next_y):
                send(last, last, bulk_send.at[q], a_recv.at[q, step], to_x)
                send(first, first, bulk_send.at[q], a_recv.at[q, step], to_y)
            first, last = last, first
        send(own, own, bulk_send.at[q], d_recv.at[q], partner)

    def relay(q):
        await_bytes(weights.at[q, pl.ds(0, 6 * 16)], a_recv.at[q, 0])
        if EVEN[q] == 2:
            await_bytes(weights.at[q, pl.ds(0, 6 * 16)], a_recv.at[q, 1])

        def forward(step, unit, targets):
            for to in targets:
                send(unit, unit, bulk_send.at[q], b_recv.at[q, step], to)

        for step, d in enumerate(STEPS):
            if d == 2 and EVEN[q] == 2:
                forward(step, unit_at(q, 0, 2), next_x[:2])
                forward(step, unit_at(q, 2, 0), next_y[:2])
                forward(step, unit_at(q, 0, 2, 0), next_x[2:])
                forward(step, unit_at(q, 2, 0, 1), next_y[2:])
            else:
                keep = 3 if d == 2 else EVEN[q]
                forward(step, unit_at(q, 0, d, 0), next_x[:keep])
                forward(step, unit_at(q, d, 0, 1), next_y[:keep])
        if EVEN[q] == 3:
            await_bytes(weights.at[q, pl.ds(0, 6 * 16)], a_recv.at[q, 1])
        for d in STEPS:
            for unit in (unit_at(q, 0, d), unit_at(q, d, 0)):
                send(unit, unit, bulk_send.at[q], d_recv.at[q], partner)

    def finish(q):
        def pass_on(i, j, half=None):
            unit = unit_at(q, i, j, half)
            send(unit, unit, bulk_send.at[q], d_recv.at[q], partner)

        for step, d in enumerate(STEPS):
            if EVEN[q] == 3:
                await_bytes(weights.at[q, pl.ds(0, 6 * 16)], b_recv.at[q, step])
                for i in (1, 3, 2):
                    pass_on(i, d, 0)
                    pass_on(d, i, 1)
            else:
                await_bytes(weights.at[q, pl.ds(0, (10 if d == 2 else 4) * 16)], b_recv.at[q, step])
                if d == 2:
                    for i in (1, 3):
                        pass_on(i, 2)
                        pass_on(2, i)
                    pass_on(2, 2)
                else:
                    for i in (1, 3):
                        pass_on(i, d, 0)
                        pass_on(d, i, 1)

    def wait_round(q):
        await_bytes(weights.at[q, pl.ds(0, RANKS * UNIT)], d_recv.at[q])

    def read_stats(p):
        await_bytes(stats.at[p, pl.ds(0, RANKS - 1)], st_recv.at[p])
        total = jnp.sum(stats[p], axis=0) * (1.0 / MEMBERS)
        mean, square = total, pltpu.roll(total, 64, 1)
        scale = lax.rsqrt(jnp.maximum(square - mean * mean, 0.0) + EPSILON)
        row = lax.broadcasted_iota(jnp.int32, (8, 128), 0)
        parts = jnp.zeros((8, 128), F32)
        for i, line in enumerate(three_parts(mean) + three_parts(scale)):
            parts = jnp.where(row == i, jnp.broadcast_to(line, (8, 128)), parts)
        lines = jnp.dot(parts[:, :64].astype(BF16), spread_out[...], preferred_element_type=F32)
        mean = (lines[0:1] + lines[1:2] + lines[2:3])[:, :C]
        scale = (lines[3:4] + lines[4:5] + lines[5:6])[:, :C]
        scale = gains[p // 2, p % 2 : p % 2 + 1, :] * scale
        offset = shifts[p // 2, p % 2 : p % 2 + 1, :] - mean * scale
        return scale * 0.5, offset * 0.5

    def normalize(p, scale, offset):
        tails = [None] * (H + 2)

        def one(i, raw, keep=None):
            v = raw.astype(F32) * scale + offset
            v = v + v * jnp.tanh(v)
            if keep is not None:
                v = jnp.where(keep, v, 0.0)
            main = v[:, :256].astype(BF16)
            tails[i] = v[:, 256:C]
            for r in range(3):
                o = i - r
                if 0 <= o < H:
                    left[o * W : (o + 1) * W, r * 256 : (r + 1) * 256] = main

        for i in range(H):
            one(i + 1, field[p, i])
        wait_halo(p)
        one(0, halo[p, 0], rank > 0)
        one(H + 1, halo[p, 1], rank < RANKS - 1)
        blank = jnp.zeros((W, 64), F32)
        for o in range(H):
            rows = slice(o * W, (o + 1) * W)
            left[rows, 768:896] = jnp.concatenate([tails[o], tails[o + 1]], axis=1).astype(BF16)
            left[rows, 896:1024] = jnp.concatenate([tails[o + 2], blank], axis=1).astype(BF16)

    edge = lax.broadcasted_iota(jnp.int32, (W, 1), 0)

    def shifted(v, t):
        if t == 1:
            return v
        if t == 0:
            return jnp.where(edge == 0, 0.0, pltpu.roll(v, 1, 0))
        return jnp.where(edge == W - 1, 0.0, pltpu.roll(v, W - 1, 0))

    def conv(p, between=None):
        s1 = jnp.zeros((8, C), F32)
        s2 = jnp.zeros((8, C), F32)
        for start in range(0, H, PART):
            band = slice(start * W, (start + PART) * W)
            for n in range(4):
                cols = slice(n * 256, (n + 1) * 256)
                prod[band, cols] = jnp.dot(left[band, :], weights[p, :, cols], preferred_element_type=F32)
            if between is not None and start + PART == H:
                between()
            for i in range(start, start + PART):
                rows = slice(i * W, (i + 1) * W)
                main, tail = 0.0, 0.0
                for t in range(3):
                    main = main + shifted(prod[rows, t * 256 : (t + 1) * 256], t)
                    tail = tail + shifted(prod[rows, 768 + 64 * t : 768 + 64 * (t + 1)], t)
                v = jnp.concatenate([main, tail], axis=1)
                if p % 2 == 1:
                    v = field[p - 1, i].astype(F32) + v
                v = v.astype(BF16)
                field[p + 1, i] = v
                v = v.astype(F32)
                s1 = s1 + fold(v)
                s2 = s2 + fold(v * v)
        return s1, s2

    def build_zero(b):
        for i in range(4):
            for t in range(3):
                k = 96 * i + 32 * t
                if k < C:
                    rows = slice((30 + i % 2) * UNIT, (31 + i % 2) * UNIT)
                    q = 2 * b + i // 2
                    zeros[b, k : k + 32, 0:256] = weights[q, rows, 256 * t : 256 * t + 256]
                    block = weights[q, rows, 768 + 128 * (t // 2) : 896 + 128 * (t // 2)].astype(F32)
                    tail = block[:, 64 * (t % 2) : 64 * (t % 2) + 64]
                    zeros[b, k : k + 32, 256:C] = tail.astype(BF16)

    def zero_conv(b):
        hidden = field[2 * b + 2].reshape(H * W, C)
        got = jnp.dot(hidden, zeros[b], preferred_element_type=F32).reshape(H, W, C)
        out[b, 0] = (got + skip_buf[b, 0].astype(F32)).astype(BF16)

    def scoped(name, f, *args):
        with jax.named_scope(name):
            return f(*args)

    scoped("s1_wait_0", wait_pieces, 0)
    scoped("assemble_0", assemble, 0)
    send_own(0)
    scoped("s1_wait_1", wait_pieces, 1)
    scoped("assemble_1", assemble, 1)
    send_own(1)
    scoped("relay_0", relay, 0)
    send_pieces(2)
    for load in load_rows:
        load.wait()
    scale, offset = scoped("stats_0", read_stats, 0)
    scoped("normalize_0", normalize, 0, scale, offset)
    scoped("finish_0", finish, 0)
    scoped("relay_1", relay, 1)
    send_pieces(3)
    scoped("wait_round_0", wait_round, 0)

    def start_2():
        wait_pieces(2)
        assemble(2)
        send_own(2)

    s1, s2 = scoped("conv_0", conv, 0, start_2)
    for p in range(1, 4):
        start_stats(p, s1, s2)
        start_halo(p)
        scoped(f"finish_{p}", finish, p)
        if p == 1:
            scoped("s1_wait_3", wait_pieces, 3)
            scoped("assemble_3", assemble, 3)
        if p < 3:
            scoped(f"relay_{p + 1}", relay, p + 1)
        if p == 1:
            send_own(3)
        if p == 2:
            load_skips.wait()
            build_zero(0)
            scoped("zero_conv_0", zero_conv, 0)
        scale, offset = scoped(f"stats_{p}", read_stats, p)
        scoped(f"normalize_{p}", normalize, p, scale, offset)
        scoped(f"wait_round_{p}", wait_round, p)
        if p == 3:
            build_zero(1)
        s1, s2 = scoped(f"conv_{p}", conv, p)
    scoped("zero_conv_1", zero_conv, 1)

    for p in range(4):
        await_bytes(stage.at[p, pl.ds(0, COL - 1)], s1_send.at[p])
        await_bytes(stats.at[p, pl.ds(0, RANKS - 1)], st_send.at[p])
        wait_halo_sends(p)
        await_bytes(weights.at[p, pl.ds(0, 992)], bulk_send.at[p])


def on_device(control, unet_skips, norm_gains, norm_shifts, conv_weights, zero_weights):
    vmem = pl.BlockSpec(memory_space=pltpu.VMEM)
    hbm = pl.BlockSpec(memory_space=pl.ANY)
    dma = pltpu.SemaphoreType.DMA
    return pl.pallas_call(
        kernel,
        out_shape=pltpu.VMEM((2, 1, H, W, C), BF16),
        in_specs=[hbm] * 6,
        out_specs=vmem,
        scratch_shapes=[
            pltpu.VMEM((2, 3, 20, 2, 3 * C), BF16),
            pltpu.VMEM((1, 20, 2, C), BF16),
            pltpu.VMEM((8, 4, 16, 128), BF16),
            pltpu.VMEM((4, LANES, LANES), BF16),
            pltpu.VMEM((4, COL, 16, 128), BF16),
            pltpu.VMEM((5, H, W, C), BF16),
            pltpu.VMEM((4, 2, W, C), BF16),
            pltpu.VMEM((H * W, LANES), BF16),
            pltpu.VMEM((H * W, LANES), F32),
            pltpu.VMEM((4, RANKS, 1, 128), F32),
            pltpu.VMEM((384, 128), BF16),
            pltpu.VMEM((64, 384), BF16),
            pltpu.VMEM((2, C, C), BF16),
            pltpu.VMEM((2, 1, H, W, C), BF16),
            pltpu.VMEM((2, 2, C), F32),
            pltpu.VMEM((2, 2, C), F32),
            dma((7,)), dma((4,)), dma((4,)),
            dma((4,)), dma((4, 2)), dma((4, 3)), dma((4,)),
            dma((4,)), dma((4,)), dma((4, 2)), dma((4, 2)),
        ],
        compiler_params=pltpu.CompilerParams(
            collective_id=0, has_side_effects=True, vmem_limit_bytes=66_150_400
        ),
    )(
        conv_weights.transpose(0, 2, 4, 1, 3), zero_weights.transpose(1, 3, 0, 2),
        control, unet_skips, norm_gains, norm_shifts,
    )


def solution(mesh):
    placed = (
        P("batch", "rows", None, None),
        P(None, "batch", "rows", None, None),
        P(),
        P(),
        P(None, None, None, None, "batch"),
        P(None, None, None, "batch"),
    )
    return jax.shard_map(
        on_device,
        mesh=mesh,
        in_specs=placed,
        out_specs=P(None, "batch", "rows", None, None),
        check_vma=False,
    )
```

```python
import jax
import jax.numpy as jnp
from jax import lax
from jax.experimental import pallas as pl
from jax.experimental.pallas import tpu as pltpu
from jax.sharding import PartitionSpec as P

MESH = pl.DeviceIdType.MESH
F32 = jnp.float32
BF16 = jnp.bfloat16
C = 320
GROUP = 10
W = 96
H = 6
SIDE = 4
RANKS = 16
COL = 16
DEPTH = 8
UNIT = 32
LANES = 1024
EVEN = (3, 2, 3, 3)
STEPS = (1, 3, 2)
PART = 2
FAR_FIRST = (
    (2, 2), (1, 2), (3, 2), (2, 1), (2, 3), (1, 1), (1, 3), (3, 1), (3, 3), (0, 2), (2, 0), (0, 1), (0, 3), (1, 0), (3, 0)
)
FAR_COLUMN = (8, 7, 9, 6, 10, 5, 11, 4, 12, 3, 13, 2, 14, 1, 15)
EPSILON = 1e-05
MEMBERS = float(96 * 96 * GROUP)


def kernel(
    taps, zero_taps, control, skips, gain_rows, shift_rows, out,
    raw, raw_zero, pieces, weights, stage, field, halo, left, prod, stats, gather, spread_out, zeros, skip_buf, gains, shifts,
    load_sem, s1_send, s1_recv, bulk_send, a_recv, b_recv, d_recv,
    st_send, st_recv, h_send, h_recv,
):
    rank = lax.axis_index("rows")
    col = lax.axis_index("batch")
    x, y = rank // SIDE, rank % SIDE
    z, core = col // 2, col % 2
    partner = (rank, 2 * z + 1 - core)

    flip_x, flip_y = (z + 1) // 2 % 2, z // 2 % 2
    z_x = lax.rem(z + 1 - 2 * (z % 2), DEPTH)
    z_y = lax.rem(z + DEPTH - 1 + 2 * (z % 2), DEPTH)

    def at_xy(i, j):
        return lax.rem(x + i, SIDE) * SIDE + lax.rem(y + j, SIDE)

    next_x = [(at_xy(1, 0), col), (at_xy(3, 0), col), (rank, 2 * z_x + core)]
    next_y = [(at_xy(0, 1), col), (at_xy(0, 3), col), (rank, 2 * z_y + core)]

    def unit_rows(i, j, half=None):
        a, b = lax.rem(x + i, SIDE), lax.rem(y + j, SIDE)
        inner = 4 * ((a // 2 + flip_x) % 2) + 2 * ((b // 2 + flip_y) % 2) + core
        start = (8 * (2 * (a % 2) + b % 2) + inner) * UNIT
        if half is None:
            return pl.ds(pl.multiple_of(start, UNIT), UNIT)
        return pl.ds(pl.multiple_of(start + half * 16, 16), 16)

    def send(src, dst, ssem, rsem, target):
        pltpu.make_async_remote_copy(
            src_ref=src, dst_ref=dst, send_sem=ssem, recv_sem=rsem,
            device_id=target, device_id_type=MESH,
        ).start()

    def await_bytes(ref, sem):
        pltpu.make_async_copy(ref, ref, sem).wait()

    barrier = pltpu.get_barrier_semaphore()
    for k in range(1, COL):
        pl.semaphore_signal(barrier, inc=1, device_id=(rank, lax.rem(col + k, COL)), device_id_type=MESH)
    for k in range(1, RANKS):
        pl.semaphore_signal(barrier, inc=1, device_id=(lax.rem(rank + k, RANKS), col), device_id_type=MESH)

    load_field = pltpu.make_async_copy(control.at[0], field.at[0], load_sem.at[0])
    load_raw = [pltpu.make_async_copy(taps.at[b], raw.at[b], load_sem.at[2 + b]) for b in range(2)]
    load_zero = pltpu.make_async_copy(zero_taps, raw_zero, load_sem.at[4])
    load_raw[0].start()
    load_zero.start()
    load_field.start()
    load_raw[1].start()
    load_skips = pltpu.make_async_copy(skips, skip_buf, load_sem.at[1])
    load_skips.start()
    load_rows = [
        pltpu.make_async_copy(gain_rows, gains, load_sem.at[5]),
        pltpu.make_async_copy(shift_rows, shifts, load_sem.at[6]),
    ]
    for load in load_rows:
        load.start()

    def belongs(shape, channels, groups):
        channel = lax.broadcasted_iota(jnp.int32, shape, channels).astype(F32)
        group = (lax.broadcasted_iota(jnp.int32, shape, groups) % 64).astype(F32)
        same = jnp.floor((channel + 0.5) * (1.0 / GROUP)) == group
        return jnp.where(same, 1.0, 0.0).astype(BF16)

    gather[...] = belongs((384, 128), 0, 1)
    spread_out[...] = belongs((64, 384), 1, 0)

    def inner_of(other):
        oz = other // 2
        fx, fy = (oz + 1) // 2 % 2, oz // 2 % 2
        return 4 * ((x // 2 + fx) % 2) + 2 * ((y // 2 + fy) % 2) + other % 2

    mine = inner_of(col)
    kind = 2 * (x % 2) + y % 2
    lane_u = lax.broadcasted_iota(jnp.int32, (16, 128), 1)

    def cut_pieces(b):
        def put(q, block, parts):
            rows = jnp.concatenate(parts + [jnp.zeros((4, 128), F32)], axis=0)
            turned = jnp.concatenate([rows.T, jnp.zeros((128, 64), F32)], axis=1)
            for k in range(4):
                low, high = turned[32 * k : 32 * k + 16], turned[32 * k + 16 : 32 * k + 32]
                both = jnp.where(lane_u < 60, low, pltpu.roll(high, 60, 1))
                pieces[4 * block + k, q] = both.astype(BF16)

        @pl.when(kind < 3)
        def _():
            both = raw[b, jnp.minimum(kind, 2)].astype(F32)
            for j in range(2):
                v = both[:, j, :]
                for block in range(2):
                    at = 128 * block
                    put(2 * b + j, block, [v[:, C * t + at : C * t + at + 128] for t in range(3)])

        @pl.when(kind == 3)
        def _():
            both = [raw[b, r].astype(F32) for r in range(3)]
            z = jnp.concatenate([raw_zero[0].astype(F32)[:, b, :], jnp.zeros((20, 64), F32)], axis=1)
            for j in range(2):
                tail = [[both[r][:, j, C * t + 256 : C * t + C] for t in range(3)] for r in range(3)]
                put(2 * b + j, 0, [jnp.concatenate([tail[0][t], tail[1][t]], axis=1) for t in range(3)])
                parts = []
                for t in range(3):
                    cuts = [z[:, 96 * (2 * j + e) + 32 * t : 96 * (2 * j + e) + 32 * t + 32] for e in range(2)]
                    parts.append(jnp.concatenate([tail[2][t]] + cuts, axis=1))
                put(2 * b + j, 1, parts)
        for j in range(2):
            stage[2 * b + j, col] = pieces[mine, 2 * b + j]

    load_raw[0].wait()
    load_zero.wait()
    with jax.named_scope("cut_0"):
        cut_pieces(0)
    load_raw[1].wait()
    with jax.named_scope("cut_1"):
        cut_pieces(1)
    for p in range(4):

        @pl.when(rank == 0)
        def _():
            halo[p, 0] = jnp.zeros((W, C), BF16)

        @pl.when(rank == RANKS - 1)
        def _():
            halo[p, 1] = jnp.zeros((W, C), BF16)

    load_field.wait()

    lane1 = lax.broadcasted_iota(jnp.int32, (1, 128), 1)

    def three_parts(v):
        parts = []
        for _ in range(3):
            part = v.astype(BF16).astype(F32)
            parts.append(part)
            v = v - part
        return parts

    def pack_stats(s1, s2):
        both = jnp.concatenate([jnp.concatenate([s1, s2], axis=0), jnp.zeros((16, 64), F32)], axis=1)
        parts = jnp.concatenate(three_parts(both), axis=0).astype(BF16)
        sums = jnp.dot(parts, gather[...], preferred_element_type=F32)
        sums = sums[0:16] + sums[16:32] + sums[32:48]
        first = jnp.sum(sums[0:8], axis=0, keepdims=True)
        second = jnp.sum(sums[8:16], axis=0, keepdims=True)
        return jnp.where(lane1 < 64, first, second)

    def start_stats(p, s1, s2):
        stats[p, rank] = pack_stats(s1, s2)
        for i, j in FAR_FIRST:
            send(stats.at[p, rank], stats.at[p, rank], st_send.at[p], st_recv.at[p], (at_xy(i, j), col))

    def start_halo(p):
        @pl.when(rank < RANKS - 1)
        def _():
            send(field.at[p, H - 1], halo.at[p, 0], h_send.at[p, 0], h_recv.at[p, 0], (rank + 1, col))

        @pl.when(rank > 0)
        def _():
            send(field.at[p, 0], halo.at[p, 1], h_send.at[p, 1], h_recv.at[p, 1], (rank - 1, col))

    def wait_halo(p):
        @pl.when(rank > 0)
        def _():
            await_bytes(halo.at[p, 0], h_recv.at[p, 0])

        @pl.when(rank < RANKS - 1)
        def _():
            await_bytes(halo.at[p, 1], h_recv.at[p, 1])

    def wait_halo_sends(p):
        @pl.when(rank < RANKS - 1)
        def _():
            await_bytes(halo.at[p, 0], h_send.at[p, 0])

        @pl.when(rank > 0)
        def _():
            await_bytes(halo.at[p, 1], h_send.at[p, 1])

    def fold(v):
        return jnp.sum(v.reshape(W // 8, 8, C), axis=0)

    s1 = jnp.zeros((8, C), F32)
    s2 = jnp.zeros((8, C), F32)
    for i in range(H):
        v = field[0, i].astype(F32)
        s1 = s1 + fold(v)
        s2 = s2 + fold(v * v)

    with jax.named_scope("barrier_wait"):
        pl.semaphore_wait(barrier, COL + RANKS - 2)

    def send_pieces(q):
        for k in FAR_COLUMN:
            to = lax.rem(col + k, COL)
            send(pieces.at[inner_of(to), q], stage.at[q, col], s1_send.at[q], s1_recv.at[q], (rank, to))

    def wait_pieces(q):
        await_bytes(stage.at[q, pl.ds(0, COL - 1)], s1_recv.at[q])

    send_pieces(0)
    start_stats(0, s1, s2)
    start_halo(0)
    send_pieces(1)
    send_pieces(2)

    def assemble(q):
        rows = [unit_rows(0, 0, h) for h in range(2)]
        acc = [[jnp.zeros((16, 128), F32) for _ in range(LANES // 128)] for _ in range(2)]
        for b in range(COL):
            piece = stage[q, b].astype(F32)
            for h in range(2):
                for t in range(3):
                    base = 60 * h + 20 * t
                    first, last = 20 * b, 20 * b + 20
                    cuts = sorted({first, last} | {n for n in (128, 256) if first < n < last})
                    rolled = {}
                    for lo, hi in zip(cuts, cuts[1:]):
                        dest = 256 * t + lo if lo < 256 else 768 + 64 * t + lo - 256
                        shift = (dest - (base + lo - first)) % 128
                        if shift not in rolled:
                            rolled[shift] = pltpu.roll(piece, shift, 1) if shift else piece
                        d, at = dest // 128, dest % 128
                        mask = (lane_u >= at) & (lane_u < at + hi - lo)
                        acc[h][d] = jnp.where(mask, rolled[shift], acc[h][d])
        for h in range(2):
            for d in range(LANES // 128):
                weights[q, rows[h], d * 128 : (d + 1) * 128] = acc[h][d].astype(BF16)

    def unit_at(q, i, j, half=None):
        return weights.at[q, unit_rows(i, j, half)]

    def send_own(q):
        own = unit_at(q, 0, 0)
        first, last = unit_at(q, 0, 0, 0), unit_at(q, 0, 0, 1)
        for step in range(2):
            for to_x, to_y in zip(next_x, next_y):
                send(last, last, bulk_send.at[q], a_recv.at[q, step], to_x)
                send(first, first, bulk_send.at[q], a_recv.at[q, step], to_y)
            first, last = last, first
        send(own, own, bulk_send.at[q], d_recv.at[q], partner)

    def relay(q):
        await_bytes(weights.at[q, pl.ds(0, 6 * 16)], a_recv.at[q, 0])
        if EVEN[q] == 2:
            await_bytes(weights.at[q, pl.ds(0, 6 * 16)], a_recv.at[q, 1])

        def forward(step, unit, targets):
            for to in targets:
                send(unit, unit, bulk_send.at[q], b_recv.at[q, step], to)

        for step, d in enumerate(STEPS):
            if d == 2 and EVEN[q] == 2:
                forward(step, unit_at(q, 0, 2), next_x[:2])
                forward(step, unit_at(q, 2, 0), next_y[:2])
                forward(step, unit_at(q, 0, 2, 0), next_x[2:])
                forward(step, unit_at(q, 2, 0, 1), next_y[2:])
            else:
                keep = 3 if d == 2 else EVEN[q]
                forward(step, unit_at(q, 0, d, 0), next_x[:keep])
                forward(step, unit_at(q, d, 0, 1), next_y[:keep])
        if EVEN[q] == 3:
            await_bytes(weights.at[q, pl.ds(0, 6 * 16)], a_recv.at[q, 1])
        for d in STEPS:
            for unit in (unit_at(q, 0, d), unit_at(q, d, 0)):
                send(unit, unit, bulk_send.at[q], d_recv.at[q], partner)

    def finish(q):
        def pass_on(i, j, half=None):
            unit = unit_at(q, i, j, half)
            send(unit, unit, bulk_send.at[q], d_recv.at[q], partner)

        for step, d in enumerate(STEPS):
            if EVEN[q] == 3:
                await_bytes(weights.at[q, pl.ds(0, 6 * 16)], b_recv.at[q, step])
                for i in (1, 3, 2):
                    pass_on(i, d, 0)
                    pass_on(d, i, 1)
            else:
                await_bytes(weights.at[q, pl.ds(0, (10 if d == 2 else 4) * 16)], b_recv.at[q, step])
                if d == 2:
                    for i in (1, 3):
                        pass_on(i, 2)
                        pass_on(2, i)
                    pass_on(2, 2)
                else:
                    for i in (1, 3):
                        pass_on(i, d, 0)
                        pass_on(d, i, 1)

    def wait_round(q):
        await_bytes(weights.at[q, pl.ds(0, RANKS * UNIT)], d_recv.at[q])

    def read_stats(p):
        await_bytes(stats.at[p, pl.ds(0, RANKS - 1)], st_recv.at[p])
        total = jnp.sum(stats[p], axis=0) * (1.0 / MEMBERS)
        mean, square = total, pltpu.roll(total, 64, 1)
        scale = lax.rsqrt(jnp.maximum(square - mean * mean, 0.0) + EPSILON)
        row = lax.broadcasted_iota(jnp.int32, (8, 128), 0)
        parts = jnp.zeros((8, 128), F32)
        for i, line in enumerate(three_parts(mean) + three_parts(scale)):
            parts = jnp.where(row == i, jnp.broadcast_to(line, (8, 128)), parts)
        lines = jnp.dot(parts[:, :64].astype(BF16), spread_out[...], preferred_element_type=F32)
        mean = (lines[0:1] + lines[1:2] + lines[2:3])[:, :C]
        scale = (lines[3:4] + lines[4:5] + lines[5:6])[:, :C]
        scale = gains[p // 2, p % 2 : p % 2 + 1, :] * scale
        offset = shifts[p // 2, p % 2 : p % 2 + 1, :] - mean * scale
        return scale * 0.5, offset * 0.5

    def normalize(p, scale, offset):
        tails = [None] * (H + 2)

        def one(i, raw, keep=None):
            v = raw.astype(F32) * scale + offset
            v = v + v * jnp.tanh(v)
            if keep is not None:
                v = jnp.where(keep, v, 0.0)
            main = v[:, :256].astype(BF16)
            tails[i] = v[:, 256:C]
            for r in range(3):
                o = i - r
                if 0 <= o < H:
                    left[o * W : (o + 1) * W, r * 256 : (r + 1) * 256] = main

        for i in range(H):
            one(i + 1, field[p, i])
        wait_halo(p)
        one(0, halo[p, 0], rank > 0)
        one(H + 1, halo[p, 1], rank < RANKS - 1)
        blank = jnp.zeros((W, 64), F32)
        for o in range(H):
            rows = slice(o * W, (o + 1) * W)
            left[rows, 768:896] = jnp.concatenate([tails[o], tails[o + 1]], axis=1).astype(BF16)
            left[rows, 896:1024] = jnp.concatenate([tails[o + 2], blank], axis=1).astype(BF16)

    edge = lax.broadcasted_iota(jnp.int32, (W, 1), 0)

    def shifted(v, t):
        if t == 1:
            return v
        if t == 0:
            return jnp.where(edge == 0, 0.0, pltpu.roll(v, 1, 0))
        return jnp.where(edge == W - 1, 0.0, pltpu.roll(v, W - 1, 0))

    def conv(p, between=None):
        sums = [jnp.zeros((8, C), F32), jnp.zeros((8, C), F32)]

        def last_row(i):
            rows = slice(i * W, (i + 1) * W)
            main, tail = 0.0, 0.0
            for t in range(3):
                main = main + shifted(prod[rows, t * 256 : (t + 1) * 256], t)
                tail = tail + shifted(prod[rows, 768 + 64 * t : 768 + 64 * (t + 1)], t)
            v = jnp.concatenate([main, tail], axis=1)
            if p % 2 == 1:
                v = field[p - 1, i].astype(F32) + v
            v = v.astype(BF16)
            field[p + 1, i] = v
            v = v.astype(F32)
            sums[0] = sums[0] + fold(v)
            sums[1] = sums[1] + fold(v * v)

        waiting = []
        for start in range(0, H, PART):
            band = slice(start * W, (start + PART) * W)
            for n in range(4):
                cols = slice(n * 256, (n + 1) * 256)
                prod[band, cols] = jnp.dot(left[band, :], weights[p, :, cols], preferred_element_type=F32)
                if waiting:
                    last_row(waiting.pop(0))
            if between is not None and start + PART == H:
                between()
            waiting += range(start, start + PART)
        for i in waiting:
            last_row(i)
        return sums

    def build_zero(b):
        for i in range(4):
            for t in range(3):
                k = 96 * i + 32 * t
                if k < C:
                    rows = slice((30 + i % 2) * UNIT, (31 + i % 2) * UNIT)
                    q = 2 * b + i // 2
                    zeros[b, k : k + 32, 0:256] = weights[q, rows, 256 * t : 256 * t + 256]
                    block = weights[q, rows, 768 + 128 * (t // 2) : 896 + 128 * (t // 2)].astype(F32)
                    tail = block[:, 64 * (t % 2) : 64 * (t % 2) + 64]
                    zeros[b, k : k + 32, 256:C] = tail.astype(BF16)

    def zero_conv(b):
        hidden = field[2 * b + 2].reshape(H * W, C)
        got = jnp.dot(hidden, zeros[b], preferred_element_type=F32).reshape(H, W, C)
        out[b, 0] = (got + skip_buf[b, 0].astype(F32)).astype(BF16)

    def scoped(name, f, *args):
        with jax.named_scope(name):
            return f(*args)

    scoped("s1_wait_0", wait_pieces, 0)
    scoped("assemble_0", assemble, 0)
    send_own(0)
    scoped("s1_wait_1", wait_pieces, 1)
    scoped("assemble_1", assemble, 1)
    send_own(1)
    scoped("relay_0", relay, 0)
    send_pieces(3)
    for load in load_rows:
        load.wait()
    scale, offset = scoped("stats_0", read_stats, 0)
    scoped("normalize_0", normalize, 0, scale, offset)
    scoped("s1_wait_2", wait_pieces, 2)
    scoped("assemble_2", assemble, 2)
    scoped("finish_0", finish, 0)
    scoped("relay_1", relay, 1)
    send_own(2)
    scoped("wait_round_0", wait_round, 0)
    s1, s2 = scoped("conv_0", conv, 0)
    for p in range(1, 4):
        start_stats(p, s1, s2)
        start_halo(p)
        scoped(f"finish_{p}", finish, p)
        if p == 1:
            scoped("s1_wait_3", wait_pieces, 3)
            scoped("assemble_3", assemble, 3)
        if p < 3:
            scoped(f"relay_{p + 1}", relay, p + 1)
        if p == 1:
            send_own(3)
        if p == 2:
            load_skips.wait()
            build_zero(0)
            scoped("zero_conv_0", zero_conv, 0)
        scale, offset = scoped(f"stats_{p}", read_stats, p)
        scoped(f"normalize_{p}", normalize, p, scale, offset)
        scoped(f"wait_round_{p}", wait_round, p)
        if p == 3:
            build_zero(1)
        s1, s2 = scoped(f"conv_{p}", conv, p)
    scoped("zero_conv_1", zero_conv, 1)

    for p in range(4):
        await_bytes(stage.at[p, pl.ds(0, COL - 1)], s1_send.at[p])
        await_bytes(stats.at[p, pl.ds(0, RANKS - 1)], st_send.at[p])
        wait_halo_sends(p)
        await_bytes(weights.at[p, pl.ds(0, 992)], bulk_send.at[p])


def on_device(control, unet_skips, norm_gains, norm_shifts, conv_weights, zero_weights):
    vmem = pl.BlockSpec(memory_space=pltpu.VMEM)
    hbm = pl.BlockSpec(memory_space=pl.ANY)
    dma = pltpu.SemaphoreType.DMA
    return pl.pallas_call(
        kernel,
        out_shape=pltpu.VMEM((2, 1, H, W, C), BF16),
        in_specs=[hbm] * 6,
        out_specs=vmem,
        scratch_shapes=[
            pltpu.VMEM((2, 3, 20, 2, 3 * C), BF16),
            pltpu.VMEM((1, 20, 2, C), BF16),
            pltpu.VMEM((8, 4, 16, 128), BF16),
            pltpu.VMEM((4, LANES, LANES), BF16),
            pltpu.VMEM((4, COL, 16, 128), BF16),
            pltpu.VMEM((5, H, W, C), BF16),
            pltpu.VMEM((4, 2, W, C), BF16),
            pltpu.VMEM((H * W, LANES), BF16),
            pltpu.VMEM((H * W, LANES), F32),
            pltpu.VMEM((4, RANKS, 1, 128), F32),
            pltpu.VMEM((384, 128), BF16),
            pltpu.VMEM((64, 384), BF16),
            pltpu.VMEM((2, C, C), BF16),
            pltpu.VMEM((2, 1, H, W, C), BF16),
            pltpu.VMEM((2, 2, C), F32),
            pltpu.VMEM((2, 2, C), F32),
            dma((7,)), dma((4,)), dma((4,)),
            dma((4,)), dma((4, 2)), dma((4, 3)), dma((4,)),
            dma((4,)), dma((4,)), dma((4, 2)), dma((4, 2)),
        ],
        compiler_params=pltpu.CompilerParams(
            collective_id=0, has_side_effects=True, vmem_limit_bytes=66_150_400
        ),
    )(
        conv_weights.transpose(0, 2, 4, 1, 3), zero_weights.transpose(1, 3, 0, 2),
        control, unet_skips, norm_gains, norm_shifts,
    )


def solution(mesh):
    placed = (
        P("batch", "rows", None, None),
        P(None, "batch", "rows", None, None),
        P(),
        P(),
        P(None, None, None, None, "batch"),
        P(None, None, None, "batch"),
    )
    return jax.shard_map(
        on_device,
        mesh=mesh,
        in_specs=placed,
        out_specs=P(None, "batch", "rows", None, None),
        check_vma=False,
    )
```

```python
import jax
import jax.numpy as jnp
from jax import lax
from jax.experimental import pallas as pl
from jax.experimental.pallas import tpu as pltpu
from jax.sharding import PartitionSpec as P

MESH = pl.DeviceIdType.MESH
F32 = jnp.float32
BF16 = jnp.bfloat16
C = 320
GROUP = 10
W = 96
H = 6
SIDE = 4
RANKS = 16
COL = 16
DEPTH = 8
UNIT = 32
LANES = 1024
EVEN = (3, 2, 3, 3)
STEPS = (1, 3, 2)
PART = 2
FAR_FIRST = (
    (2, 2), (1, 2), (3, 2), (2, 1), (2, 3), (1, 1), (1, 3), (3, 1), (3, 3), (0, 2), (2, 0), (0, 1), (0, 3), (1, 0), (3, 0)
)
FAR_COLUMN = (8, 7, 9, 6, 10, 5, 11, 4, 12, 3, 13, 2, 14, 1, 15)
EPSILON = 1e-05
MEMBERS = float(96 * 96 * GROUP)


def kernel(
    taps, zero_taps, control, skips, gain_rows, shift_rows, out,
    raw, raw_zero, pieces, weights, stage, field, halo, left, prod, stats, gather, spread_out, zeros, skip_buf, gains, shifts,
    load_sem, s1_send, s1_recv, bulk_send, a_recv, b_recv, d_recv,
    st_send, st_recv, h_send, h_recv,
):
    rank = lax.axis_index("rows")
    col = lax.axis_index("batch")
    x, y = rank // SIDE, rank % SIDE
    z, core = col // 2, col % 2
    partner = (rank, 2 * z + 1 - core)

    flip_x, flip_y = (z + 1) // 2 % 2, z // 2 % 2
    z_x = lax.rem(z + 1 - 2 * (z % 2), DEPTH)
    z_y = lax.rem(z + DEPTH - 1 + 2 * (z % 2), DEPTH)

    def at_xy(i, j):
        return lax.rem(x + i, SIDE) * SIDE + lax.rem(y + j, SIDE)

    next_x = [(at_xy(1, 0), col), (at_xy(3, 0), col), (rank, 2 * z_x + core)]
    next_y = [(at_xy(0, 1), col), (at_xy(0, 3), col), (rank, 2 * z_y + core)]

    starts = {}
    for i in range(SIDE):
        for j in range(SIDE):
            a, b = lax.rem(x + i, SIDE), lax.rem(y + j, SIDE)
            inner = 4 * ((a // 2 + flip_x) % 2) + 2 * ((b // 2 + flip_y) % 2) + core
            starts[i, j] = (8 * (2 * (a % 2) + b % 2) + inner) * UNIT

    def unit_rows(i, j, half=None):
        start = starts[i, j]
        if half is None:
            return pl.ds(pl.multiple_of(start, UNIT), UNIT)
        return pl.ds(pl.multiple_of(start + half * 16, 16), 16)

    def send(src, dst, ssem, rsem, target):
        pltpu.make_async_remote_copy(
            src_ref=src, dst_ref=dst, send_sem=ssem, recv_sem=rsem,
            device_id=target, device_id_type=MESH,
        ).start()

    def await_bytes(ref, sem):
        pltpu.make_async_copy(ref, ref, sem).wait()

    barrier = pltpu.get_barrier_semaphore()
    column = [lax.rem(col + k, COL) for k in FAR_COLUMN]
    plane = [at_xy(i, j) for i, j in FAR_FIRST]
    for to, r in zip(column, plane):
        pl.semaphore_signal(barrier, inc=1, device_id=(rank, to), device_id_type=MESH)
        pl.semaphore_signal(barrier, inc=1, device_id=(r, col), device_id_type=MESH)

    load_field = pltpu.make_async_copy(control.at[0], field.at[0], load_sem.at[0])
    load_raw = [pltpu.make_async_copy(taps.at[b], raw.at[b], load_sem.at[2 + b]) for b in range(2)]
    load_zero = pltpu.make_async_copy(zero_taps, raw_zero, load_sem.at[4])
    load_raw[0].start()
    load_zero.start()
    load_field.start()
    load_raw[1].start()
    load_skips = pltpu.make_async_copy(skips, skip_buf, load_sem.at[1])
    load_skips.start()
    load_rows = [
        pltpu.make_async_copy(gain_rows, gains, load_sem.at[5]),
        pltpu.make_async_copy(shift_rows, shifts, load_sem.at[6]),
    ]
    for load in load_rows:
        load.start()

    def belongs(shape, channels, groups):
        channel = lax.broadcasted_iota(jnp.int32, shape, channels).astype(F32)
        group = (lax.broadcasted_iota(jnp.int32, shape, groups) % 64).astype(F32)
        same = jnp.floor((channel + 0.5) * (1.0 / GROUP)) == group
        return jnp.where(same, 1.0, 0.0).astype(BF16)

    gather[...] = belongs((384, 128), 0, 1)
    spread_out[...] = belongs((64, 384), 1, 0)

    def inner_of(other):
        oz = other // 2
        fx, fy = (oz + 1) // 2 % 2, oz // 2 % 2
        return 4 * ((x // 2 + fx) % 2) + 2 * ((y // 2 + fy) % 2) + other % 2

    mine = inner_of(col)
    column_inner = [inner_of(to) for to in column]
    kind = 2 * (x % 2) + y % 2
    lane_u = lax.broadcasted_iota(jnp.int32, (16, 128), 1)

    def cut_pieces(b):
        def put(q, block, parts):
            rows = jnp.concatenate(parts + [jnp.zeros((4, 128), F32)], axis=0)
            turned = jnp.concatenate([rows.T, jnp.zeros((128, 64), F32)], axis=1)
            for k in range(4):
                low, high = turned[32 * k : 32 * k + 16], turned[32 * k + 16 : 32 * k + 32]
                both = jnp.where(lane_u < 60, low, pltpu.roll(high, 60, 1))
                pieces[4 * block + k, q] = both.astype(BF16)

        @pl.when(kind < 3)
        def _():
            both = raw[b, jnp.minimum(kind, 2)].astype(F32)
            for j in range(2):
                v = both[:, j, :]
                for block in range(2):
                    at = 128 * block
                    put(2 * b + j, block, [v[:, C * t + at : C * t + at + 128] for t in range(3)])

        @pl.when(kind == 3)
        def _():
            both = [raw[b, r].astype(F32) for r in range(3)]
            z = jnp.concatenate([raw_zero[0].astype(F32)[:, b, :], jnp.zeros((20, 64), F32)], axis=1)
            for j in range(2):
                tail = [[both[r][:, j, C * t + 256 : C * t + C] for t in range(3)] for r in range(3)]
                put(2 * b + j, 0, [jnp.concatenate([tail[0][t], tail[1][t]], axis=1) for t in range(3)])
                parts = []
                for t in range(3):
                    cuts = [z[:, 96 * (2 * j + e) + 32 * t : 96 * (2 * j + e) + 32 * t + 32] for e in range(2)]
                    parts.append(jnp.concatenate([tail[2][t]] + cuts, axis=1))
                put(2 * b + j, 1, parts)
        for j in range(2):
            stage[2 * b + j, col] = pieces[mine, 2 * b + j]

    load_raw[0].wait()
    load_zero.wait()
    with jax.named_scope("cut_0"):
        cut_pieces(0)
    load_raw[1].wait()
    with jax.named_scope("cut_1"):
        cut_pieces(1)
    for p in range(4):

        @pl.when(rank == 0)
        def _():
            halo[p, 0] = jnp.zeros((W, C), BF16)

        @pl.when(rank == RANKS - 1)
        def _():
            halo[p, 1] = jnp.zeros((W, C), BF16)

    load_field.wait()

    lane1 = lax.broadcasted_iota(jnp.int32, (1, 128), 1)

    def three_parts(v):
        parts = []
        for _ in range(3):
            part = v.astype(BF16).astype(F32)
            parts.append(part)
            v = v - part
        return parts

    def pack_stats(s1, s2):
        both = jnp.concatenate([jnp.concatenate([s1, s2], axis=0), jnp.zeros((16, 64), F32)], axis=1)
        parts = jnp.concatenate(three_parts(both), axis=0).astype(BF16)
        sums = jnp.dot(parts, gather[...], preferred_element_type=F32)
        sums = sums[0:16] + sums[16:32] + sums[32:48]
        first = jnp.sum(sums[0:8], axis=0, keepdims=True)
        second = jnp.sum(sums[8:16], axis=0, keepdims=True)
        return jnp.where(lane1 < 64, first, second)

    def start_stats(p, s1, s2):
        stats[p, rank] = pack_stats(s1, s2)
        for r in plane:
            send(stats.at[p, rank], stats.at[p, rank], st_send.at[p], st_recv.at[p], (r, col))

    def start_halo(p):
        @pl.when(rank < RANKS - 1)
        def _():
            send(field.at[p, H - 1], halo.at[p, 0], h_send.at[p, 0], h_recv.at[p, 0], (rank + 1, col))

        @pl.when(rank > 0)
        def _():
            send(field.at[p, 0], halo.at[p, 1], h_send.at[p, 1], h_recv.at[p, 1], (rank - 1, col))

    def wait_halo(p):
        @pl.when(rank > 0)
        def _():
            await_bytes(halo.at[p, 0], h_recv.at[p, 0])

        @pl.when(rank < RANKS - 1)
        def _():
            await_bytes(halo.at[p, 1], h_recv.at[p, 1])

    def wait_halo_sends(p):
        @pl.when(rank < RANKS - 1)
        def _():
            await_bytes(halo.at[p, 0], h_send.at[p, 0])

        @pl.when(rank > 0)
        def _():
            await_bytes(halo.at[p, 1], h_send.at[p, 1])

    def fold(v):
        return jnp.sum(v.reshape(W // 8, 8, C), axis=0)

    s1 = jnp.zeros((8, C), F32)
    s2 = jnp.zeros((8, C), F32)
    for i in range(H):
        v = field[0, i].astype(F32)
        s1 = s1 + fold(v)
        s2 = s2 + fold(v * v)

    with jax.named_scope("barrier_wait"):
        pl.semaphore_wait(barrier, COL + RANKS - 2)

    def send_pieces(q):
        for to, inner in zip(column, column_inner):
            send(pieces.at[inner, q], stage.at[q, col], s1_send.at[q], s1_recv.at[q], (rank, to))

    def wait_pieces(q):
        await_bytes(stage.at[q, pl.ds(0, COL - 1)], s1_recv.at[q])

    send_pieces(0)
    start_stats(0, s1, s2)
    start_halo(0)
    send_pieces(1)
    send_pieces(2)

    def assemble(q):
        rows = [unit_rows(0, 0, h) for h in range(2)]
        acc = [[jnp.zeros((16, 128), F32) for _ in range(LANES // 128)] for _ in range(2)]
        for b in range(COL):
            piece = stage[q, b].astype(F32)
            for h in range(2):
                for t in range(3):
                    base = 60 * h + 20 * t
                    first, last = 20 * b, 20 * b + 20
                    cuts = sorted({first, last} | {n for n in (128, 256) if first < n < last})
                    rolled = {}
                    for lo, hi in zip(cuts, cuts[1:]):
                        dest = 256 * t + lo if lo < 256 else 768 + 64 * t + lo - 256
                        shift = (dest - (base + lo - first)) % 128
                        if shift not in rolled:
                            rolled[shift] = pltpu.roll(piece, shift, 1) if shift else piece
                        d, at = dest // 128, dest % 128
                        mask = (lane_u >= at) & (lane_u < at + hi - lo)
                        acc[h][d] = jnp.where(mask, rolled[shift], acc[h][d])
        for h in range(2):
            for d in range(LANES // 128):
                weights[q, rows[h], d * 128 : (d + 1) * 128] = acc[h][d].astype(BF16)

    def unit_at(q, i, j, half=None):
        return weights.at[q, unit_rows(i, j, half)]

    def send_own(q):
        own = unit_at(q, 0, 0)
        first, last = unit_at(q, 0, 0, 0), unit_at(q, 0, 0, 1)
        for step in range(2):
            for to_x, to_y in zip(next_x, next_y):
                send(last, last, bulk_send.at[q], a_recv.at[q, step], to_x)
                send(first, first, bulk_send.at[q], a_recv.at[q, step], to_y)
            first, last = last, first
        send(own, own, bulk_send.at[q], d_recv.at[q], partner)

    def relay(q):
        await_bytes(weights.at[q, pl.ds(0, 6 * 16)], a_recv.at[q, 0])
        if EVEN[q] == 2:
            await_bytes(weights.at[q, pl.ds(0, 6 * 16)], a_recv.at[q, 1])

        def forward(step, unit, targets):
            for to in targets:
                send(unit, unit, bulk_send.at[q], b_recv.at[q, step], to)

        for step, d in enumerate(STEPS):
            if d == 2 and EVEN[q] == 2:
                forward(step, unit_at(q, 0, 2), next_x[:2])
                forward(step, unit_at(q, 2, 0), next_y[:2])
                forward(step, unit_at(q, 0, 2, 0), next_x[2:])
                forward(step, unit_at(q, 2, 0, 1), next_y[2:])
            else:
                keep = 3 if d == 2 else EVEN[q]
                forward(step, unit_at(q, 0, d, 0), next_x[:keep])
                forward(step, unit_at(q, d, 0, 1), next_y[:keep])
        if EVEN[q] == 3:
            await_bytes(weights.at[q, pl.ds(0, 6 * 16)], a_recv.at[q, 1])
        for d in STEPS:
            for unit in (unit_at(q, 0, d), unit_at(q, d, 0)):
                send(unit, unit, bulk_send.at[q], d_recv.at[q], partner)

    def finish(q):
        def pass_on(i, j, half=None):
            unit = unit_at(q, i, j, half)
            send(unit, unit, bulk_send.at[q], d_recv.at[q], partner)

        for step, d in enumerate(STEPS):
            if EVEN[q] == 3:
                await_bytes(weights.at[q, pl.ds(0, 6 * 16)], b_recv.at[q, step])
                for i in (1, 3, 2):
                    pass_on(i, d, 0)
                    pass_on(d, i, 1)
            else:
                await_bytes(weights.at[q, pl.ds(0, (10 if d == 2 else 4) * 16)], b_recv.at[q, step])
                if d == 2:
                    for i in (1, 3):
                        pass_on(i, 2)
                        pass_on(2, i)
                    pass_on(2, 2)
                else:
                    for i in (1, 3):
                        pass_on(i, d, 0)
                        pass_on(d, i, 1)

    def wait_round(q):
        await_bytes(weights.at[q, pl.ds(0, RANKS * UNIT)], d_recv.at[q])

    def read_stats(p):
        await_bytes(stats.at[p, pl.ds(0, RANKS - 1)], st_recv.at[p])
        total = jnp.sum(stats[p], axis=0) * (1.0 / MEMBERS)
        mean, square = total, pltpu.roll(total, 64, 1)
        scale = lax.rsqrt(jnp.maximum(square - mean * mean, 0.0) + EPSILON)
        row = lax.broadcasted_iota(jnp.int32, (8, 128), 0)
        parts = jnp.zeros((8, 128), F32)
        for i, line in enumerate(three_parts(mean) + three_parts(scale)):
            parts = jnp.where(row == i, jnp.broadcast_to(line, (8, 128)), parts)
        lines = jnp.dot(parts[:, :64].astype(BF16), spread_out[...], preferred_element_type=F32)
        mean = (lines[0:1] + lines[1:2] + lines[2:3])[:, :C]
        scale = (lines[3:4] + lines[4:5] + lines[5:6])[:, :C]
        scale = gains[p // 2, p % 2 : p % 2 + 1, :] * scale
        offset = shifts[p // 2, p % 2 : p % 2 + 1, :] - mean * scale
        return scale * 0.5, offset * 0.5

    def normalize(p, scale, offset):
        tails = [None] * (H + 2)

        def one(i, raw, keep=None):
            v = raw.astype(F32) * scale + offset
            v = v + v * jnp.tanh(v)
            if keep is not None:
                v = jnp.where(keep, v, 0.0)
            main = v[:, :256].astype(BF16)
            tails[i] = v[:, 256:C]
            for r in range(3):
                o = i - r
                if 0 <= o < H:
                    left[o * W : (o + 1) * W, r * 256 : (r + 1) * 256] = main

        for i in range(H):
            one(i + 1, field[p, i])
        wait_halo(p)
        one(0, halo[p, 0], rank > 0)
        one(H + 1, halo[p, 1], rank < RANKS - 1)
        blank = jnp.zeros((W, 64), F32)
        for o in range(H):
            rows = slice(o * W, (o + 1) * W)
            left[rows, 768:896] = jnp.concatenate([tails[o], tails[o + 1]], axis=1).astype(BF16)
            left[rows, 896:1024] = jnp.concatenate([tails[o + 2], blank], axis=1).astype(BF16)

    edge = lax.broadcasted_iota(jnp.int32, (W, 1), 0)

    def shifted(v, t):
        if t == 1:
            return v
        if t == 0:
            return jnp.where(edge == 0, 0.0, pltpu.roll(v, 1, 0))
        return jnp.where(edge == W - 1, 0.0, pltpu.roll(v, W - 1, 0))

    def conv(p, between=None):
        sums = [jnp.zeros((8, C), F32), jnp.zeros((8, C), F32)]

        def last_row(i):
            rows = slice(i * W, (i + 1) * W)
            main, tail = 0.0, 0.0
            for t in range(3):
                main = main + shifted(prod[rows, t * 256 : (t + 1) * 256], t)
                tail = tail + shifted(prod[rows, 768 + 64 * t : 768 + 64 * (t + 1)], t)
            v = jnp.concatenate([main, tail], axis=1)
            if p % 2 == 1:
                v = field[p - 1, i].astype(F32) + v
            v = v.astype(BF16)
            field[p + 1, i] = v
            v = v.astype(F32)
            sums[0] = sums[0] + fold(v)
            sums[1] = sums[1] + fold(v * v)

        waiting = []
        for start in range(0, H, PART):
            band = slice(start * W, (start + PART) * W)
            for n in range(4):
                cols = slice(n * 256, (n + 1) * 256)
                prod[band, cols] = jnp.dot(left[band, :], weights[p, :, cols], preferred_element_type=F32)
                if waiting:
                    last_row(waiting.pop(0))
            if between is not None and start + PART == H:
                between()
            waiting += range(start, start + PART)
        for i in waiting:
            last_row(i)
        return sums

    def build_zero(b):
        for i in range(4):
            for t in range(3):
                k = 96 * i + 32 * t
                if k < C:
                    rows = slice((30 + i % 2) * UNIT, (31 + i % 2) * UNIT)
                    q = 2 * b + i // 2
                    zeros[b, k : k + 32, 0:256] = weights[q, rows, 256 * t : 256 * t + 256]
                    block = weights[q, rows, 768 + 128 * (t // 2) : 896 + 128 * (t // 2)].astype(F32)
                    tail = block[:, 64 * (t % 2) : 64 * (t % 2) + 64]
                    zeros[b, k : k + 32, 256:C] = tail.astype(BF16)

    def zero_conv(b):
        hidden = field[2 * b + 2].reshape(H * W, C)
        got = jnp.dot(hidden, zeros[b], preferred_element_type=F32).reshape(H, W, C)
        out[b, 0] = (got + skip_buf[b, 0].astype(F32)).astype(BF16)

    def scoped(name, f, *args):
        with jax.named_scope(name):
            return f(*args)

    scoped("s1_wait_0", wait_pieces, 0)
    scoped("assemble_0", assemble, 0)
    send_own(0)
    scoped("s1_wait_1", wait_pieces, 1)
    scoped("assemble_1", assemble, 1)
    send_own(1)
    scoped("relay_0", relay, 0)
    send_pieces(3)
    for load in load_rows:
        load.wait()
    scale, offset = scoped("stats_0", read_stats, 0)
    scoped("normalize_0", normalize, 0, scale, offset)
    scoped("s1_wait_2", wait_pieces, 2)
    scoped("assemble_2", assemble, 2)
    scoped("finish_0", finish, 0)
    scoped("relay_1", relay, 1)
    send_own(2)
    scoped("wait_round_0", wait_round, 0)
    s1, s2 = scoped("conv_0", conv, 0)
    for p in range(1, 4):
        start_stats(p, s1, s2)
        start_halo(p)
        scoped(f"finish_{p}", finish, p)
        if p == 1:
            scoped("s1_wait_3", wait_pieces, 3)
            scoped("assemble_3", assemble, 3)
        if p < 3:
            scoped(f"relay_{p + 1}", relay, p + 1)
        if p == 1:
            send_own(3)
        if p == 2:
            load_skips.wait()
            build_zero(0)
            scoped("zero_conv_0", zero_conv, 0)
        scale, offset = scoped(f"stats_{p}", read_stats, p)
        scoped(f"normalize_{p}", normalize, p, scale, offset)
        scoped(f"wait_round_{p}", wait_round, p)
        if p == 3:
            build_zero(1)
        s1, s2 = scoped(f"conv_{p}", conv, p)
    scoped("zero_conv_1", zero_conv, 1)

    for p in range(4):
        await_bytes(stage.at[p, pl.ds(0, COL - 1)], s1_send.at[p])
        await_bytes(stats.at[p, pl.ds(0, RANKS - 1)], st_send.at[p])
        wait_halo_sends(p)
        await_bytes(weights.at[p, pl.ds(0, 992)], bulk_send.at[p])


def on_device(control, unet_skips, norm_gains, norm_shifts, conv_weights, zero_weights):
    vmem = pl.BlockSpec(memory_space=pltpu.VMEM)
    hbm = pl.BlockSpec(memory_space=pl.ANY)
    dma = pltpu.SemaphoreType.DMA
    return pl.pallas_call(
        kernel,
        out_shape=pltpu.VMEM((2, 1, H, W, C), BF16),
        in_specs=[hbm] * 6,
        out_specs=vmem,
        scratch_shapes=[
            pltpu.VMEM((2, 3, 20, 2, 3 * C), BF16),
            pltpu.VMEM((1, 20, 2, C), BF16),
            pltpu.VMEM((8, 4, 16, 128), BF16),
            pltpu.VMEM((4, LANES, LANES), BF16),
            pltpu.VMEM((4, COL, 16, 128), BF16),
            pltpu.VMEM((5, H, W, C), BF16),
            pltpu.VMEM((4, 2, W, C), BF16),
            pltpu.VMEM((H * W, LANES), BF16),
            pltpu.VMEM((H * W, LANES), F32),
            pltpu.VMEM((4, RANKS, 1, 128), F32),
            pltpu.VMEM((384, 128), BF16),
            pltpu.VMEM((64, 384), BF16),
            pltpu.VMEM((2, C, C), BF16),
            pltpu.VMEM((2, 1, H, W, C), BF16),
            pltpu.VMEM((2, 2, C), F32),
            pltpu.VMEM((2, 2, C), F32),
            dma((7,)), dma((4,)), dma((4,)),
            dma((4,)), dma((4, 2)), dma((4, 3)), dma((4,)),
            dma((4,)), dma((4,)), dma((4, 2)), dma((4, 2)),
        ],
        compiler_params=pltpu.CompilerParams(
            collective_id=0, has_side_effects=True, vmem_limit_bytes=66_150_400
        ),
    )(
        conv_weights.transpose(0, 2, 4, 1, 3), zero_weights.transpose(1, 3, 0, 2),
        control, unet_skips, norm_gains, norm_shifts,
    )


def solution(mesh):
    placed = (
        P("batch", "rows", None, None),
        P(None, "batch", "rows", None, None),
        P(),
        P(),
        P(None, None, None, None, "batch"),
        P(None, None, None, "batch"),
    )
    return jax.shard_map(
        on_device,
        mesh=mesh,
        in_specs=placed,
        out_specs=P(None, "batch", "rows", None, None),
        check_vma=False,
    )
```

```python
import jax
import jax.numpy as jnp
from jax import lax
from jax.experimental import pallas as pl
from jax.experimental.pallas import tpu as pltpu
from jax.sharding import PartitionSpec as P

MESH = pl.DeviceIdType.MESH
F32 = jnp.float32
BF16 = jnp.bfloat16
C = 320
GROUP = 10
W = 96
H = 6
SIDE = 4
RANKS = 16
COL = 16
DEPTH = 8
UNIT = 32
LANES = 1024
EVEN = (3, 3, 3, 3)
STEPS = (1, 3, 2)
PART = 2
FAR_FIRST = (
    (2, 2), (1, 2), (3, 2), (2, 1), (2, 3), (1, 1), (1, 3), (3, 1), (3, 3), (0, 2), (2, 0), (0, 1), (0, 3), (1, 0), (3, 0)
)
FAR_COLUMN = (8, 7, 9, 6, 10, 5, 11, 4, 12, 3, 13, 2, 14, 1, 15)
EPSILON = 1e-05
MEMBERS = float(96 * 96 * GROUP)


def kernel(
    taps, zero_taps, control, skips, gain_rows, shift_rows, out,
    raw, raw_zero, pieces, weights, stage, field, halo, left, prod, stats, gather, spread_out, zeros, skip_buf, gains, shifts,
    load_sem, s1_send, s1_recv, bulk_send, a_recv, b_recv, d_recv,
    st_send, st_recv, h_send, h_recv,
):
    rank = lax.axis_index("rows")
    col = lax.axis_index("batch")
    x, y = rank // SIDE, rank % SIDE
    z, core = col // 2, col % 2
    partner = (rank, 2 * z + 1 - core)

    flip_x, flip_y = (z + 1) // 2 % 2, z // 2 % 2
    z_x = lax.rem(z + 1 - 2 * (z % 2), DEPTH)
    z_y = lax.rem(z + DEPTH - 1 + 2 * (z % 2), DEPTH)

    def at_xy(i, j):
        return lax.rem(x + i, SIDE) * SIDE + lax.rem(y + j, SIDE)

    next_x = [(at_xy(1, 0), col), (at_xy(3, 0), col), (rank, 2 * z_x + core)]
    next_y = [(at_xy(0, 1), col), (at_xy(0, 3), col), (rank, 2 * z_y + core)]

    starts = {}
    for i in range(SIDE):
        for j in range(SIDE):
            a, b = lax.rem(x + i, SIDE), lax.rem(y + j, SIDE)
            inner = 4 * ((a // 2 + flip_x) % 2) + 2 * ((b // 2 + flip_y) % 2) + core
            starts[i, j] = (8 * (2 * (a % 2) + b % 2) + inner) * UNIT

    def unit_rows(i, j, half=None):
        start = starts[i, j]
        if half is None:
            return pl.ds(pl.multiple_of(start, UNIT), UNIT)
        return pl.ds(pl.multiple_of(start + half * 16, 16), 16)

    def send(src, dst, ssem, rsem, target):
        pltpu.make_async_remote_copy(
            src_ref=src, dst_ref=dst, send_sem=ssem, recv_sem=rsem,
            device_id=target, device_id_type=MESH,
        ).start()

    def await_bytes(ref, sem):
        pltpu.make_async_copy(ref, ref, sem).wait()

    barrier = pltpu.get_barrier_semaphore()
    column = [lax.rem(col + k, COL) for k in FAR_COLUMN]
    plane = [at_xy(i, j) for i, j in FAR_FIRST]
    for to, r in zip(column, plane):
        pl.semaphore_signal(barrier, inc=1, device_id=(rank, to), device_id_type=MESH)
        pl.semaphore_signal(barrier, inc=1, device_id=(r, col), device_id_type=MESH)

    load_field = pltpu.make_async_copy(control.at[0], field.at[0], load_sem.at[0])
    load_raw = [pltpu.make_async_copy(taps.at[b], raw.at[b], load_sem.at[2 + b]) for b in range(2)]
    load_zero = pltpu.make_async_copy(zero_taps, raw_zero, load_sem.at[4])
    load_raw[0].start()
    load_zero.start()
    load_field.start()
    load_raw[1].start()
    load_skips = pltpu.make_async_copy(skips, skip_buf, load_sem.at[1])
    load_skips.start()
    load_rows = [
        pltpu.make_async_copy(gain_rows, gains, load_sem.at[5]),
        pltpu.make_async_copy(shift_rows, shifts, load_sem.at[6]),
    ]
    for load in load_rows:
        load.start()

    def belongs(shape, channels, groups):
        channel = lax.broadcasted_iota(jnp.int32, shape, channels).astype(F32)
        group = (lax.broadcasted_iota(jnp.int32, shape, groups) % 64).astype(F32)
        same = jnp.floor((channel + 0.5) * (1.0 / GROUP)) == group
        return jnp.where(same, 1.0, 0.0).astype(BF16)

    gather[...] = belongs((384, 128), 0, 1)
    spread_out[...] = belongs((64, 384), 1, 0)

    def inner_of(other):
        oz = other // 2
        fx, fy = (oz + 1) // 2 % 2, oz // 2 % 2
        return 4 * ((x // 2 + fx) % 2) + 2 * ((y // 2 + fy) % 2) + other % 2

    mine = inner_of(col)
    column_inner = [inner_of(to) for to in column]
    kind = 2 * (x % 2) + y % 2
    lane_u = lax.broadcasted_iota(jnp.int32, (16, 128), 1)

    def cut_pieces(b):
        def put(q, block, parts):
            rows = jnp.concatenate(parts + [jnp.zeros((4, 128), F32)], axis=0)
            turned = jnp.concatenate([rows.T, jnp.zeros((128, 64), F32)], axis=1)
            for k in range(4):
                low, high = turned[32 * k : 32 * k + 16], turned[32 * k + 16 : 32 * k + 32]
                both = jnp.where(lane_u < 60, low, pltpu.roll(high, 60, 1))
                pieces[4 * block + k, q] = both.astype(BF16)

        @pl.when(kind < 3)
        def _():
            both = raw[b, jnp.minimum(kind, 2)].astype(F32)
            for j in range(2):
                v = both[:, j, :]
                for block in range(2):
                    at = 128 * block
                    put(2 * b + j, block, [v[:, C * t + at : C * t + at + 128] for t in range(3)])

        @pl.when(kind == 3)
        def _():
            both = [raw[b, r].astype(F32) for r in range(3)]
            z = jnp.concatenate([raw_zero[0].astype(F32)[:, b, :], jnp.zeros((20, 64), F32)], axis=1)
            for j in range(2):
                tail = [[both[r][:, j, C * t + 256 : C * t + C] for t in range(3)] for r in range(3)]
                put(2 * b + j, 0, [jnp.concatenate([tail[0][t], tail[1][t]], axis=1) for t in range(3)])
                parts = []
                for t in range(3):
                    cuts = [z[:, 96 * (2 * j + e) + 32 * t : 96 * (2 * j + e) + 32 * t + 32] for e in range(2)]
                    parts.append(jnp.concatenate([tail[2][t]] + cuts, axis=1))
                put(2 * b + j, 1, parts)
        for j in range(2):
            stage[2 * b + j, col] = pieces[mine, 2 * b + j]

    load_raw[0].wait()
    load_zero.wait()
    with jax.named_scope("cut_0"):
        cut_pieces(0)
    load_raw[1].wait()
    with jax.named_scope("cut_1"):
        cut_pieces(1)
    for p in range(4):

        @pl.when(rank == 0)
        def _():
            halo[p, 0] = jnp.zeros((W, C), BF16)

        @pl.when(rank == RANKS - 1)
        def _():
            halo[p, 1] = jnp.zeros((W, C), BF16)

    load_field.wait()

    lane1 = lax.broadcasted_iota(jnp.int32, (1, 128), 1)

    def three_parts(v):
        parts = []
        for _ in range(3):
            part = v.astype(BF16).astype(F32)
            parts.append(part)
            v = v - part
        return parts

    def pack_stats(s1, s2):
        both = jnp.concatenate([jnp.concatenate([s1, s2], axis=0), jnp.zeros((16, 64), F32)], axis=1)
        parts = jnp.concatenate(three_parts(both), axis=0).astype(BF16)
        sums = jnp.dot(parts, gather[...], preferred_element_type=F32)
        sums = sums[0:16] + sums[16:32] + sums[32:48]
        first = jnp.sum(sums[0:8], axis=0, keepdims=True)
        second = jnp.sum(sums[8:16], axis=0, keepdims=True)
        return jnp.where(lane1 < 64, first, second)

    def start_stats(p, s1, s2):
        stats[p, rank] = pack_stats(s1, s2)
        for r in plane:
            send(stats.at[p, rank], stats.at[p, rank], st_send.at[p], st_recv.at[p], (r, col))

    def start_halo(p):
        @pl.when(rank < RANKS - 1)
        def _():
            send(field.at[p, H - 1], halo.at[p, 0], h_send.at[p, 0], h_recv.at[p, 0], (rank + 1, col))

        @pl.when(rank > 0)
        def _():
            send(field.at[p, 0], halo.at[p, 1], h_send.at[p, 1], h_recv.at[p, 1], (rank - 1, col))

    def wait_halo(p):
        @pl.when(rank > 0)
        def _():
            await_bytes(halo.at[p, 0], h_recv.at[p, 0])

        @pl.when(rank < RANKS - 1)
        def _():
            await_bytes(halo.at[p, 1], h_recv.at[p, 1])

    def wait_halo_sends(p):
        @pl.when(rank < RANKS - 1)
        def _():
            await_bytes(halo.at[p, 0], h_send.at[p, 0])

        @pl.when(rank > 0)
        def _():
            await_bytes(halo.at[p, 1], h_send.at[p, 1])

    def fold(v):
        return jnp.sum(v.reshape(W // 8, 8, C), axis=0)

    s1 = jnp.zeros((8, C), F32)
    s2 = jnp.zeros((8, C), F32)
    for i in range(H):
        v = field[0, i].astype(F32)
        s1 = s1 + fold(v)
        s2 = s2 + fold(v * v)

    with jax.named_scope("barrier_wait"):
        pl.semaphore_wait(barrier, COL + RANKS - 2)

    def send_pieces(q):
        for to, inner in zip(column, column_inner):
            send(pieces.at[inner, q], stage.at[q, col], s1_send.at[q], s1_recv.at[q], (rank, to))

    def wait_pieces(q):
        await_bytes(stage.at[q, pl.ds(0, COL - 1)], s1_recv.at[q])

    send_pieces(0)
    start_stats(0, s1, s2)
    start_halo(0)
    send_pieces(1)
    send_pieces(2)

    def assemble(q):
        rows = [unit_rows(0, 0, h) for h in range(2)]
        acc = [[jnp.zeros((16, 128), F32) for _ in range(LANES // 128)] for _ in range(2)]
        for b in range(COL):
            piece = stage[q, b].astype(F32)
            for h in range(2):
                for t in range(3):
                    base = 60 * h + 20 * t
                    first, last = 20 * b, 20 * b + 20
                    cuts = sorted({first, last} | {n for n in (128, 256) if first < n < last})
                    rolled = {}
                    for lo, hi in zip(cuts, cuts[1:]):
                        dest = 256 * t + lo if lo < 256 else 768 + 64 * t + lo - 256
                        shift = (dest - (base + lo - first)) % 128
                        if shift not in rolled:
                            rolled[shift] = pltpu.roll(piece, shift, 1) if shift else piece
                        d, at = dest // 128, dest % 128
                        mask = (lane_u >= at) & (lane_u < at + hi - lo)
                        acc[h][d] = jnp.where(mask, rolled[shift], acc[h][d])
        for h in range(2):
            for d in range(LANES // 128):
                weights[q, rows[h], d * 128 : (d + 1) * 128] = acc[h][d].astype(BF16)

    def unit_at(q, i, j, half=None):
        return weights.at[q, unit_rows(i, j, half)]

    def send_own(q):
        own = unit_at(q, 0, 0)
        first, last = unit_at(q, 0, 0, 0), unit_at(q, 0, 0, 1)
        for step in range(2):
            for to_x, to_y in zip(next_x, next_y):
                send(last, last, bulk_send.at[q], a_recv.at[q, step], to_x)
                send(first, first, bulk_send.at[q], a_recv.at[q, step], to_y)
            first, last = last, first
        send(own, own, bulk_send.at[q], d_recv.at[q], partner)

    def relay(q):
        await_bytes(weights.at[q, pl.ds(0, 6 * 16)], a_recv.at[q, 0])
        if EVEN[q] == 2:
            await_bytes(weights.at[q, pl.ds(0, 6 * 16)], a_recv.at[q, 1])

        def forward(step, unit, targets):
            for to in targets:
                send(unit, unit, bulk_send.at[q], b_recv.at[q, step], to)

        for step, d in enumerate(STEPS):
            if d == 2 and EVEN[q] == 2:
                forward(step, unit_at(q, 0, 2), next_x[:2])
                forward(step, unit_at(q, 2, 0), next_y[:2])
                forward(step, unit_at(q, 0, 2, 0), next_x[2:])
                forward(step, unit_at(q, 2, 0, 1), next_y[2:])
            else:
                keep = 3 if d == 2 else EVEN[q]
                forward(step, unit_at(q, 0, d, 0), next_x[:keep])
                forward(step, unit_at(q, d, 0, 1), next_y[:keep])
        if EVEN[q] == 3:
            await_bytes(weights.at[q, pl.ds(0, 6 * 16)], a_recv.at[q, 1])
        for d in STEPS:
            for unit in (unit_at(q, 0, d), unit_at(q, d, 0)):
                send(unit, unit, bulk_send.at[q], d_recv.at[q], partner)

    def finish(q):
        def pass_on(i, j, half=None):
            unit = unit_at(q, i, j, half)
            send(unit, unit, bulk_send.at[q], d_recv.at[q], partner)

        for step, d in enumerate(STEPS):
            if EVEN[q] == 3:
                await_bytes(weights.at[q, pl.ds(0, 6 * 16)], b_recv.at[q, step])
                for i in (1, 3, 2):
                    pass_on(i, d, 0)
                    pass_on(d, i, 1)
            else:
                await_bytes(weights.at[q, pl.ds(0, (10 if d == 2 else 4) * 16)], b_recv.at[q, step])
                if d == 2:
                    for i in (1, 3):
                        pass_on(i, 2)
                        pass_on(2, i)
                    pass_on(2, 2)
                else:
                    for i in (1, 3):
                        pass_on(i, d, 0)
                        pass_on(d, i, 1)

    def wait_round(q):
        await_bytes(weights.at[q, pl.ds(0, RANKS * UNIT)], d_recv.at[q])

    def read_stats(p):
        await_bytes(stats.at[p, pl.ds(0, RANKS - 1)], st_recv.at[p])
        total = jnp.sum(stats[p], axis=0) * (1.0 / MEMBERS)
        mean, square = total, pltpu.roll(total, 64, 1)
        scale = lax.rsqrt(jnp.maximum(square - mean * mean, 0.0) + EPSILON)
        row = lax.broadcasted_iota(jnp.int32, (8, 128), 0)
        parts = jnp.zeros((8, 128), F32)
        for i, line in enumerate(three_parts(mean) + three_parts(scale)):
            parts = jnp.where(row == i, jnp.broadcast_to(line, (8, 128)), parts)
        lines = jnp.dot(parts[:, :64].astype(BF16), spread_out[...], preferred_element_type=F32)
        mean = (lines[0:1] + lines[1:2] + lines[2:3])[:, :C]
        scale = (lines[3:4] + lines[4:5] + lines[5:6])[:, :C]
        scale = gains[p // 2, p % 2 : p % 2 + 1, :] * scale
        offset = shifts[p // 2, p % 2 : p % 2 + 1, :] - mean * scale
        return scale * 0.5, offset * 0.5

    def normalize(p, scale, offset):
        tails = [None] * (H + 2)

        def one(i, raw, keep=None):
            v = raw.astype(F32) * scale + offset
            v = v + v * jnp.tanh(v)
            if keep is not None:
                v = jnp.where(keep, v, 0.0)
            main = v[:, :256].astype(BF16)
            tails[i] = v[:, 256:C]
            for r in range(3):
                o = i - r
                if 0 <= o < H:
                    left[o * W : (o + 1) * W, r * 256 : (r + 1) * 256] = main

        for i in range(H):
            one(i + 1, field[p, i])
        wait_halo(p)
        one(0, halo[p, 0], rank > 0)
        one(H + 1, halo[p, 1], rank < RANKS - 1)
        blank = jnp.zeros((W, 64), F32)
        for o in range(H):
            rows = slice(o * W, (o + 1) * W)
            left[rows, 768:896] = jnp.concatenate([tails[o], tails[o + 1]], axis=1).astype(BF16)
            left[rows, 896:1024] = jnp.concatenate([tails[o + 2], blank], axis=1).astype(BF16)

    edge = lax.broadcasted_iota(jnp.int32, (W, 1), 0)

    def shifted(v, t):
        if t == 1:
            return v
        if t == 0:
            return jnp.where(edge == 0, 0.0, pltpu.roll(v, 1, 0))
        return jnp.where(edge == W - 1, 0.0, pltpu.roll(v, W - 1, 0))

    def conv(p, between=None):
        sums = [jnp.zeros((8, C), F32), jnp.zeros((8, C), F32)]

        def last_row(i):
            rows = slice(i * W, (i + 1) * W)
            main, tail = 0.0, 0.0
            for t in range(3):
                main = main + shifted(prod[rows, t * 256 : (t + 1) * 256], t)
                tail = tail + shifted(prod[rows, 768 + 64 * t : 768 + 64 * (t + 1)], t)
            v = jnp.concatenate([main, tail], axis=1)
            if p % 2 == 1:
                v = field[p - 1, i].astype(F32) + v
            v = v.astype(BF16)
            field[p + 1, i] = v
            v = v.astype(F32)
            sums[0] = sums[0] + fold(v)
            sums[1] = sums[1] + fold(v * v)

        waiting = []
        for start in range(0, H, PART):
            band = slice(start * W, (start + PART) * W)
            for n in range(4):
                cols = slice(n * 256, (n + 1) * 256)
                prod[band, cols] = jnp.dot(left[band, :], weights[p, :, cols], preferred_element_type=F32)
                if waiting:
                    last_row(waiting.pop(0))
                    if p == 3 and not waiting:
                        zero_conv(1, start - PART, start)
            if between is not None and start + PART == H:
                between()
            waiting += range(start, start + PART)
        for i in waiting:
            last_row(i)
        if p == 3:
            zero_conv(1, H - PART, H)
        return sums

    def build_zero(b):
        for i in range(4):
            for t in range(3):
                k = 96 * i + 32 * t
                if k < C:
                    rows = slice((30 + i % 2) * UNIT, (31 + i % 2) * UNIT)
                    q = 2 * b + i // 2
                    zeros[b, k : k + 32, 0:256] = weights[q, rows, 256 * t : 256 * t + 256]
                    block = weights[q, rows, 768 + 128 * (t // 2) : 896 + 128 * (t // 2)].astype(F32)
                    tail = block[:, 64 * (t % 2) : 64 * (t % 2) + 64]
                    zeros[b, k : k + 32, 256:C] = tail.astype(BF16)

    def zero_conv(b, first, last):
        hidden = field[2 * b + 2, first:last].reshape((last - first) * W, C)
        got = jnp.dot(hidden, zeros[b], preferred_element_type=F32).reshape(last - first, W, C)
        out[b, 0, first:last] = (got + skip_buf[b, 0, first:last].astype(F32)).astype(BF16)

    def scoped(name, f, *args):
        with jax.named_scope(name):
            return f(*args)

    scoped("s1_wait_0", wait_pieces, 0)
    scoped("assemble_0", assemble, 0)
    send_own(0)
    scoped("s1_wait_1", wait_pieces, 1)
    scoped("assemble_1", assemble, 1)
    send_own(1)
    scoped("relay_0", relay, 0)
    send_pieces(3)
    for load in load_rows:
        load.wait()
    scale, offset = scoped("stats_0", read_stats, 0)
    scoped("normalize_0", normalize, 0, scale, offset)
    scoped("s1_wait_2", wait_pieces, 2)
    scoped("assemble_2", assemble, 2)
    scoped("finish_0", finish, 0)
    scoped("relay_1", relay, 1)
    send_own(2)
    scoped("wait_round_0", wait_round, 0)
    s1, s2 = scoped("conv_0", conv, 0)
    for p in range(1, 4):
        start_stats(p, s1, s2)
        start_halo(p)
        scoped(f"finish_{p}", finish, p)
        if p == 1:
            scoped("s1_wait_3", wait_pieces, 3)
            scoped("assemble_3", assemble, 3)
        if p < 3:
            scoped(f"relay_{p + 1}", relay, p + 1)
        if p == 1:
            send_own(3)
        if p == 2:
            load_skips.wait()
            build_zero(0)
            scoped("zero_conv_0", zero_conv, 0, 0, H)
        scale, offset = scoped(f"stats_{p}", read_stats, p)
        scoped(f"normalize_{p}", normalize, p, scale, offset)
        scoped(f"wait_round_{p}", wait_round, p)
        if p == 3:
            build_zero(1)
        s1, s2 = scoped(f"conv_{p}", conv, p)

    for p in range(4):
        await_bytes(stage.at[p, pl.ds(0, COL - 1)], s1_send.at[p])
        await_bytes(stats.at[p, pl.ds(0, RANKS - 1)], st_send.at[p])
        wait_halo_sends(p)
        await_bytes(weights.at[p, pl.ds(0, 992)], bulk_send.at[p])


def on_device(control, unet_skips, norm_gains, norm_shifts, conv_weights, zero_weights):
    vmem = pl.BlockSpec(memory_space=pltpu.VMEM)
    hbm = pl.BlockSpec(memory_space=pl.ANY)
    dma = pltpu.SemaphoreType.DMA
    return pl.pallas_call(
        kernel,
        out_shape=pltpu.VMEM((2, 1, H, W, C), BF16),
        in_specs=[hbm] * 6,
        out_specs=vmem,
        scratch_shapes=[
            pltpu.VMEM((2, 3, 20, 2, 3 * C), BF16),
            pltpu.VMEM((1, 20, 2, C), BF16),
            pltpu.VMEM((8, 4, 16, 128), BF16),
            pltpu.VMEM((4, LANES, LANES), BF16),
            pltpu.VMEM((4, COL, 16, 128), BF16),
            pltpu.VMEM((5, H, W, C), BF16),
            pltpu.VMEM((4, 2, W, C), BF16),
            pltpu.VMEM((H * W, LANES), BF16),
            pltpu.VMEM((H * W, LANES), F32),
            pltpu.VMEM((4, RANKS, 1, 128), F32),
            pltpu.VMEM((384, 128), BF16),
            pltpu.VMEM((64, 384), BF16),
            pltpu.VMEM((2, C, C), BF16),
            pltpu.VMEM((2, 1, H, W, C), BF16),
            pltpu.VMEM((2, 2, C), F32),
            pltpu.VMEM((2, 2, C), F32),
            dma((7,)), dma((4,)), dma((4,)),
            dma((4,)), dma((4, 2)), dma((4, 3)), dma((4,)),
            dma((4,)), dma((4,)), dma((4, 2)), dma((4, 2)),
        ],
        compiler_params=pltpu.CompilerParams(
            collective_id=0, has_side_effects=True, vmem_limit_bytes=66_150_400
        ),
    )(
        conv_weights.transpose(0, 2, 4, 1, 3), zero_weights.transpose(1, 3, 0, 2),
        control, unet_skips, norm_gains, norm_shifts,
    )


def solution(mesh):
    placed = (
        P("batch", "rows", None, None),
        P(None, "batch", "rows", None, None),
        P(),
        P(),
        P(None, None, None, None, "batch"),
        P(None, None, None, "batch"),
    )
    return jax.shard_map(
        on_device,
        mesh=mesh,
        in_specs=placed,
        out_specs=P(None, "batch", "rows", None, None),
        check_vma=False,
    )
```

```python
import jax
import jax.numpy as jnp
from jax import lax
from jax.experimental import pallas as pl
from jax.experimental.pallas import tpu as pltpu
from jax.sharding import PartitionSpec as P

MESH = pl.DeviceIdType.MESH
F32 = jnp.float32
BF16 = jnp.bfloat16
C = 320
GROUP = 10
W = 96
H = 6
SIDE = 4
RANKS = 16
COL = 16
DEPTH = 8
UNIT = 32
LANES = 1024
EVEN = (3, 3, 3, 3)
STEPS = (1, 3, 2)
PART = 2
FAR_FIRST = (
    (2, 2), (1, 2), (3, 2), (2, 1), (2, 3), (1, 1), (1, 3), (3, 1), (3, 3), (0, 2), (2, 0), (0, 1), (0, 3), (1, 0), (3, 0)
)
FAR_COLUMN = (8, 7, 9, 6, 10, 5, 11, 4, 12, 3, 13, 2, 14, 1, 15)
EPSILON = 1e-05
MEMBERS = float(96 * 96 * GROUP)


def kernel(
    taps, zero_taps, control, skips, gain_rows, shift_rows, out,
    raw, raw_zero, pieces, weights, stage, field, halo, left, prod, stats, gather, spread_out, zeros, skip_buf, gains, shifts,
    load_sem, s1_send, s1_recv, bulk_send, a_recv, b_recv, d_recv,
    st_send, st_recv, h_send, h_recv,
):
    rank = lax.axis_index("rows")
    col = lax.axis_index("batch")
    x, y = rank // SIDE, rank % SIDE
    z, core = col // 2, col % 2
    partner = (rank, 2 * z + 1 - core)

    flip_x, flip_y = (z + 1) // 2 % 2, z // 2 % 2
    z_x = lax.rem(z + 1 - 2 * (z % 2), DEPTH)
    z_y = lax.rem(z + DEPTH - 1 + 2 * (z % 2), DEPTH)

    def at_xy(i, j):
        return lax.rem(x + i, SIDE) * SIDE + lax.rem(y + j, SIDE)

    next_x = [(at_xy(1, 0), col), (at_xy(3, 0), col), (rank, 2 * z_x + core)]
    next_y = [(at_xy(0, 1), col), (at_xy(0, 3), col), (rank, 2 * z_y + core)]

    starts = {}
    for i in range(SIDE):
        for j in range(SIDE):
            a, b = lax.rem(x + i, SIDE), lax.rem(y + j, SIDE)
            inner = 4 * ((a // 2 + flip_x) % 2) + 2 * ((b // 2 + flip_y) % 2) + core
            starts[i, j] = (8 * (2 * (a % 2) + b % 2) + inner) * UNIT

    def unit_rows(i, j, half=None):
        start = starts[i, j]
        if half is None:
            return pl.ds(pl.multiple_of(start, UNIT), UNIT)
        return pl.ds(pl.multiple_of(start + half * 16, 16), 16)

    def send(src, dst, ssem, rsem, target):
        pltpu.make_async_remote_copy(
            src_ref=src, dst_ref=dst, send_sem=ssem, recv_sem=rsem,
            device_id=target, device_id_type=MESH,
        ).start()

    def await_bytes(ref, sem):
        pltpu.make_async_copy(ref, ref, sem).wait()

    barrier = pltpu.get_barrier_semaphore()
    column = [lax.rem(col + k, COL) for k in FAR_COLUMN]
    plane = [at_xy(i, j) for i, j in FAR_FIRST]
    for to, r in zip(column, plane):
        pl.semaphore_signal(barrier, inc=1, device_id=(rank, to), device_id_type=MESH)
        pl.semaphore_signal(barrier, inc=1, device_id=(r, col), device_id_type=MESH)

    load_field = pltpu.make_async_copy(control.at[0], field.at[0], load_sem.at[0])
    load_raw = [pltpu.make_async_copy(taps.at[b], raw.at[b], load_sem.at[2 + b]) for b in range(2)]
    load_zero = pltpu.make_async_copy(zero_taps, raw_zero, load_sem.at[4])
    load_raw[0].start()
    load_zero.start()
    load_field.start()
    load_raw[1].start()
    load_skips = pltpu.make_async_copy(skips, skip_buf, load_sem.at[1])
    load_skips.start()
    load_rows = [
        pltpu.make_async_copy(gain_rows, gains, load_sem.at[5]),
        pltpu.make_async_copy(shift_rows, shifts, load_sem.at[6]),
    ]
    for load in load_rows:
        load.start()

    def belongs(shape, channels, groups):
        channel = lax.broadcasted_iota(jnp.int32, shape, channels).astype(F32)
        group = (lax.broadcasted_iota(jnp.int32, shape, groups) % 64).astype(F32)
        same = jnp.floor((channel + 0.5) * (1.0 / GROUP)) == group
        return jnp.where(same, 1.0, 0.0).astype(BF16)

    gather[...] = belongs((384, 128), 0, 1)
    spread_out[...] = belongs((64, 384), 1, 0)

    def inner_of(other):
        oz = other // 2
        fx, fy = (oz + 1) // 2 % 2, oz // 2 % 2
        return 4 * ((x // 2 + fx) % 2) + 2 * ((y // 2 + fy) % 2) + other % 2

    mine = inner_of(col)
    column_inner = [inner_of(to) for to in column]
    kind = 2 * (x % 2) + y % 2
    lane_u = lax.broadcasted_iota(jnp.int32, (16, 128), 1)

    def cut_pieces(b):
        def put(q, block, parts):
            rows = jnp.concatenate(parts + [jnp.zeros((4, 128), F32)], axis=0)
            turned = jnp.concatenate([rows.T, jnp.zeros((128, 64), F32)], axis=1)
            for k in range(4):
                low, high = turned[32 * k : 32 * k + 16], turned[32 * k + 16 : 32 * k + 32]
                both = jnp.where(lane_u < 60, low, pltpu.roll(high, 60, 1))
                pieces[4 * block + k, q] = both.astype(BF16)

        @pl.when(kind < 3)
        def _():
            both = raw[b, jnp.minimum(kind, 2)].astype(F32)
            for j in range(2):
                v = both[:, j, :]
                for block in range(2):
                    at = 128 * block
                    put(2 * b + j, block, [v[:, C * t + at : C * t + at + 128] for t in range(3)])

        @pl.when(kind == 3)
        def _():
            both = [raw[b, r].astype(F32) for r in range(3)]
            z = jnp.concatenate([raw_zero[0].astype(F32)[:, b, :], jnp.zeros((20, 64), F32)], axis=1)
            for j in range(2):
                tail = [[both[r][:, j, C * t + 256 : C * t + C] for t in range(3)] for r in range(3)]
                put(2 * b + j, 0, [jnp.concatenate([tail[0][t], tail[1][t]], axis=1) for t in range(3)])
                parts = []
                for t in range(3):
                    cuts = [z[:, 96 * (2 * j + e) + 32 * t : 96 * (2 * j + e) + 32 * t + 32] for e in range(2)]
                    parts.append(jnp.concatenate([tail[2][t]] + cuts, axis=1))
                put(2 * b + j, 1, parts)
        for j in range(2):
            stage[2 * b + j, col] = pieces[mine, 2 * b + j]

    load_raw[0].wait()
    load_zero.wait()
    with jax.named_scope("cut_0"):
        cut_pieces(0)
    load_raw[1].wait()
    with jax.named_scope("cut_1"):
        cut_pieces(1)
    for p in range(4):

        @pl.when(rank == 0)
        def _():
            halo[p, 0] = jnp.zeros((W, C), BF16)

        @pl.when(rank == RANKS - 1)
        def _():
            halo[p, 1] = jnp.zeros((W, C), BF16)

    load_field.wait()

    lane1 = lax.broadcasted_iota(jnp.int32, (1, 128), 1)

    def three_parts(v):
        parts = []
        for _ in range(3):
            part = v.astype(BF16).astype(F32)
            parts.append(part)
            v = v - part
        return parts

    def pack_stats(s1, s2):
        both = jnp.concatenate([jnp.concatenate([s1, s2], axis=0), jnp.zeros((16, 64), F32)], axis=1)
        parts = jnp.concatenate(three_parts(both), axis=0).astype(BF16)
        sums = jnp.dot(parts, gather[...], preferred_element_type=F32)
        sums = sums[0:16] + sums[16:32] + sums[32:48]
        first = jnp.sum(sums[0:8], axis=0, keepdims=True)
        second = jnp.sum(sums[8:16], axis=0, keepdims=True)
        return jnp.where(lane1 < 64, first, second)

    def start_stats(p, s1, s2):
        stats[p, rank] = pack_stats(s1, s2)
        for r in plane:
            send(stats.at[p, rank], stats.at[p, rank], st_send.at[p], st_recv.at[p], (r, col))

    def start_halo(p):
        @pl.when(rank < RANKS - 1)
        def _():
            send(field.at[p, H - 1], halo.at[p, 0], h_send.at[p, 0], h_recv.at[p, 0], (rank + 1, col))

        @pl.when(rank > 0)
        def _():
            send(field.at[p, 0], halo.at[p, 1], h_send.at[p, 1], h_recv.at[p, 1], (rank - 1, col))

    def wait_halo(p):
        @pl.when(rank > 0)
        def _():
            await_bytes(halo.at[p, 0], h_recv.at[p, 0])

        @pl.when(rank < RANKS - 1)
        def _():
            await_bytes(halo.at[p, 1], h_recv.at[p, 1])

    def wait_halo_sends(p):
        @pl.when(rank < RANKS - 1)
        def _():
            await_bytes(halo.at[p, 0], h_send.at[p, 0])

        @pl.when(rank > 0)
        def _():
            await_bytes(halo.at[p, 1], h_send.at[p, 1])

    def fold(v):
        return jnp.sum(v.reshape(W // 8, 8, C), axis=0)

    s1 = jnp.zeros((8, C), F32)
    s2 = jnp.zeros((8, C), F32)
    for i in range(H):
        v = field[0, i].astype(F32)
        s1 = s1 + fold(v)
        s2 = s2 + fold(v * v)

    with jax.named_scope("barrier_wait"):
        pl.semaphore_wait(barrier, COL + RANKS - 2)

    def send_pieces(q):
        for to, inner in zip(column, column_inner):
            send(pieces.at[inner, q], stage.at[q, col], s1_send.at[q], s1_recv.at[q], (rank, to))

    def wait_pieces(q):
        await_bytes(stage.at[q, pl.ds(0, COL - 1)], s1_recv.at[q])

    send_pieces(0)
    start_stats(0, s1, s2)
    start_halo(0)
    send_pieces(1)
    send_pieces(2)

    def assemble(q):
        rows = [unit_rows(0, 0, h) for h in range(2)]
        acc = [[jnp.zeros((16, 128), F32) for _ in range(LANES // 128)] for _ in range(2)]
        for b in range(COL):
            piece = stage[q, b].astype(F32)
            for h in range(2):
                for t in range(3):
                    base = 60 * h + 20 * t
                    first, last = 20 * b, 20 * b + 20
                    cuts = sorted({first, last} | {n for n in (128, 256) if first < n < last})
                    rolled = {}
                    for lo, hi in zip(cuts, cuts[1:]):
                        dest = 256 * t + lo if lo < 256 else 768 + 64 * t + lo - 256
                        shift = (dest - (base + lo - first)) % 128
                        if shift not in rolled:
                            rolled[shift] = pltpu.roll(piece, shift, 1) if shift else piece
                        d, at = dest // 128, dest % 128
                        mask = (lane_u >= at) & (lane_u < at + hi - lo)
                        acc[h][d] = jnp.where(mask, rolled[shift], acc[h][d])
        for h in range(2):
            for d in range(LANES // 128):
                weights[q, rows[h], d * 128 : (d + 1) * 128] = acc[h][d].astype(BF16)

    def unit_at(q, i, j, half=None):
        return weights.at[q, unit_rows(i, j, half)]

    def send_own(q):
        own = unit_at(q, 0, 0)
        first, last = unit_at(q, 0, 0, 0), unit_at(q, 0, 0, 1)
        for step in range(2):
            for to_x, to_y in zip(next_x, next_y):
                send(last, last, bulk_send.at[q], a_recv.at[q, step], to_x)
                send(first, first, bulk_send.at[q], a_recv.at[q, step], to_y)
            first, last = last, first
        send(own, own, bulk_send.at[q], d_recv.at[q], partner)

    def relay(q):
        await_bytes(weights.at[q, pl.ds(0, 6 * 16)], a_recv.at[q, 0])
        if EVEN[q] == 2:
            await_bytes(weights.at[q, pl.ds(0, 6 * 16)], a_recv.at[q, 1])

        def forward(step, unit, targets):
            for to in targets:
                send(unit, unit, bulk_send.at[q], b_recv.at[q, step], to)

        for step, d in enumerate(STEPS):
            if d == 2 and EVEN[q] == 2:
                forward(step, unit_at(q, 0, 2), next_x[:2])
                forward(step, unit_at(q, 2, 0), next_y[:2])
                forward(step, unit_at(q, 0, 2, 0), next_x[2:])
                forward(step, unit_at(q, 2, 0, 1), next_y[2:])
            else:
                keep = 3 if d == 2 else EVEN[q]
                forward(step, unit_at(q, 0, d, 0), next_x[:keep])
                forward(step, unit_at(q, d, 0, 1), next_y[:keep])
        if EVEN[q] == 3:
            await_bytes(weights.at[q, pl.ds(0, 6 * 16)], a_recv.at[q, 1])
        for d in STEPS:
            for unit in (unit_at(q, 0, d), unit_at(q, d, 0)):
                send(unit, unit, bulk_send.at[q], d_recv.at[q], partner)

    def finish(q, steps=(0, 1, 2)):
        def pass_on(i, j, half=None):
            unit = unit_at(q, i, j, half)
            send(unit, unit, bulk_send.at[q], d_recv.at[q], partner)

        for step in steps:
            d = STEPS[step]
            if EVEN[q] == 3:
                await_bytes(weights.at[q, pl.ds(0, 6 * 16)], b_recv.at[q, step])
                for i in (1, 3, 2):
                    pass_on(i, d, 0)
                    pass_on(d, i, 1)
            else:
                await_bytes(weights.at[q, pl.ds(0, (10 if d == 2 else 4) * 16)], b_recv.at[q, step])
                if d == 2:
                    for i in (1, 3):
                        pass_on(i, 2)
                        pass_on(2, i)
                    pass_on(2, 2)
                else:
                    for i in (1, 3):
                        pass_on(i, d, 0)
                        pass_on(d, i, 1)

    def wait_round(q):
        await_bytes(weights.at[q, pl.ds(0, RANKS * UNIT)], d_recv.at[q])

    def read_stats(p):
        await_bytes(stats.at[p, pl.ds(0, RANKS - 1)], st_recv.at[p])
        total = jnp.sum(stats[p], axis=0) * (1.0 / MEMBERS)
        mean, square = total, pltpu.roll(total, 64, 1)
        scale = lax.rsqrt(jnp.maximum(square - mean * mean, 0.0) + EPSILON)
        row = lax.broadcasted_iota(jnp.int32, (8, 128), 0)
        parts = jnp.zeros((8, 128), F32)
        for i, line in enumerate(three_parts(mean) + three_parts(scale)):
            parts = jnp.where(row == i, jnp.broadcast_to(line, (8, 128)), parts)
        lines = jnp.dot(parts[:, :64].astype(BF16), spread_out[...], preferred_element_type=F32)
        mean = (lines[0:1] + lines[1:2] + lines[2:3])[:, :C]
        scale = (lines[3:4] + lines[4:5] + lines[5:6])[:, :C]
        scale = gains[p // 2, p % 2 : p % 2 + 1, :] * scale
        offset = shifts[p // 2, p % 2 : p % 2 + 1, :] - mean * scale
        return scale * 0.5, offset * 0.5

    def normalize(p, scale, offset):
        tails = [None] * (H + 2)

        def one(i, raw, keep=None):
            v = raw.astype(F32) * scale + offset
            v = v + v * jnp.tanh(v)
            if keep is not None:
                v = jnp.where(keep, v, 0.0)
            main = v[:, :256].astype(BF16)
            tails[i] = v[:, 256:C]
            for r in range(3):
                o = i - r
                if 0 <= o < H:
                    left[o * W : (o + 1) * W, r * 256 : (r + 1) * 256] = main

        for i in range(H):
            one(i + 1, field[p, i])
        wait_halo(p)
        one(0, halo[p, 0], rank > 0)
        one(H + 1, halo[p, 1], rank < RANKS - 1)
        blank = jnp.zeros((W, 64), F32)
        for o in range(H):
            rows = slice(o * W, (o + 1) * W)
            left[rows, 768:896] = jnp.concatenate([tails[o], tails[o + 1]], axis=1).astype(BF16)
            left[rows, 896:1024] = jnp.concatenate([tails[o + 2], blank], axis=1).astype(BF16)

    edge = lax.broadcasted_iota(jnp.int32, (W, 1), 0)

    def shifted(v, t):
        if t == 1:
            return v
        if t == 0:
            return jnp.where(edge == 0, 0.0, pltpu.roll(v, 1, 0))
        return jnp.where(edge == W - 1, 0.0, pltpu.roll(v, W - 1, 0))

    def conv(p, between=None):
        sums = [jnp.zeros((8, C), F32), jnp.zeros((8, C), F32)]

        def last_row(i):
            rows = slice(i * W, (i + 1) * W)
            main, tail = 0.0, 0.0
            for t in range(3):
                main = main + shifted(prod[rows, t * 256 : (t + 1) * 256], t)
                tail = tail + shifted(prod[rows, 768 + 64 * t : 768 + 64 * (t + 1)], t)
            v = jnp.concatenate([main, tail], axis=1)
            if p % 2 == 1:
                v = field[p - 1, i].astype(F32) + v
            v = v.astype(BF16)
            field[p + 1, i] = v
            v = v.astype(F32)
            sums[0] = sums[0] + fold(v)
            sums[1] = sums[1] + fold(v * v)

        waiting = []
        for start in range(0, H, PART):
            band = slice(start * W, (start + PART) * W)
            for n in range(4):
                cols = slice(n * 256, (n + 1) * 256)
                prod[band, cols] = jnp.dot(left[band, :], weights[p, :, cols], preferred_element_type=F32)
                if waiting:
                    last_row(waiting.pop(0))
                    if p == 3 and not waiting:
                        zero_conv(1, start - PART, start)
            if between is not None and start + PART == H:
                between()
            waiting += range(start, start + PART)
        for i in waiting:
            last_row(i)
        if p == 3:
            zero_conv(1, H - PART, H)
        return sums

    def build_zero(b):
        for i in range(4):
            for t in range(3):
                k = 96 * i + 32 * t
                if k < C:
                    rows = slice((30 + i % 2) * UNIT, (31 + i % 2) * UNIT)
                    q = 2 * b + i // 2
                    zeros[b, k : k + 32, 0:256] = weights[q, rows, 256 * t : 256 * t + 256]
                    block = weights[q, rows, 768 + 128 * (t // 2) : 896 + 128 * (t // 2)].astype(F32)
                    tail = block[:, 64 * (t % 2) : 64 * (t % 2) + 64]
                    zeros[b, k : k + 32, 256:C] = tail.astype(BF16)

    def zero_conv(b, first, last):
        hidden = field[2 * b + 2, first:last].reshape((last - first) * W, C)
        got = jnp.dot(hidden, zeros[b], preferred_element_type=F32).reshape(last - first, W, C)
        out[b, 0, first:last] = (got + skip_buf[b, 0, first:last].astype(F32)).astype(BF16)

    def scoped(name, f, *args):
        with jax.named_scope(name):
            return f(*args)

    scoped("s1_wait_0", wait_pieces, 0)
    scoped("assemble_0", assemble, 0)
    send_own(0)
    scoped("s1_wait_1", wait_pieces, 1)
    scoped("assemble_1", assemble, 1)
    send_own(1)
    scoped("relay_0", relay, 0)
    send_pieces(3)
    for load in load_rows:
        load.wait()
    scale, offset = scoped("stats_0", read_stats, 0)
    scoped("normalize_0", normalize, 0, scale, offset)
    scoped("s1_wait_2", wait_pieces, 2)
    scoped("assemble_2", assemble, 2)
    finish(0, (0, 1))
    scoped("relay_1", relay, 1)
    scoped("finish_0", finish, 0, (2,))
    send_own(2)
    scoped("wait_round_0", wait_round, 0)
    s1, s2 = scoped("conv_0", conv, 0)
    for p in range(1, 4):
        start_stats(p, s1, s2)
        start_halo(p)
        scoped(f"finish_{p}", finish, p)
        if p == 1:
            scoped("s1_wait_3", wait_pieces, 3)
            scoped("assemble_3", assemble, 3)
        if p < 3:
            scoped(f"relay_{p + 1}", relay, p + 1)
        if p == 1:
            send_own(3)
        if p == 2:
            load_skips.wait()
            build_zero(0)
            scoped("zero_conv_0", zero_conv, 0, 0, H)
        scale, offset = scoped(f"stats_{p}", read_stats, p)
        scoped(f"normalize_{p}", normalize, p, scale, offset)
        scoped(f"wait_round_{p}", wait_round, p)
        if p == 3:
            build_zero(1)
        s1, s2 = scoped(f"conv_{p}", conv, p)

    for p in range(4):
        await_bytes(stage.at[p, pl.ds(0, COL - 1)], s1_send.at[p])
        await_bytes(stats.at[p, pl.ds(0, RANKS - 1)], st_send.at[p])
        wait_halo_sends(p)
        await_bytes(weights.at[p, pl.ds(0, 992)], bulk_send.at[p])


def on_device(control, unet_skips, norm_gains, norm_shifts, conv_weights, zero_weights):
    vmem = pl.BlockSpec(memory_space=pltpu.VMEM)
    hbm = pl.BlockSpec(memory_space=pl.ANY)
    dma = pltpu.SemaphoreType.DMA
    return pl.pallas_call(
        kernel,
        out_shape=pltpu.VMEM((2, 1, H, W, C), BF16),
        in_specs=[hbm] * 6,
        out_specs=vmem,
        scratch_shapes=[
            pltpu.VMEM((2, 3, 20, 2, 3 * C), BF16),
            pltpu.VMEM((1, 20, 2, C), BF16),
            pltpu.VMEM((8, 4, 16, 128), BF16),
            pltpu.VMEM((4, LANES, LANES), BF16),
            pltpu.VMEM((4, COL, 16, 128), BF16),
            pltpu.VMEM((5, H, W, C), BF16),
            pltpu.VMEM((4, 2, W, C), BF16),
            pltpu.VMEM((H * W, LANES), BF16),
            pltpu.VMEM((H * W, LANES), F32),
            pltpu.VMEM((4, RANKS, 1, 128), F32),
            pltpu.VMEM((384, 128), BF16),
            pltpu.VMEM((64, 384), BF16),
            pltpu.VMEM((2, C, C), BF16),
            pltpu.VMEM((2, 1, H, W, C), BF16),
            pltpu.VMEM((2, 2, C), F32),
            pltpu.VMEM((2, 2, C), F32),
            dma((7,)), dma((4,)), dma((4,)),
            dma((4,)), dma((4, 2)), dma((4, 3)), dma((4,)),
            dma((4,)), dma((4,)), dma((4, 2)), dma((4, 2)),
        ],
        compiler_params=pltpu.CompilerParams(
            collective_id=0, has_side_effects=True, vmem_limit_bytes=66_150_400
        ),
    )(
        conv_weights.transpose(0, 2, 4, 1, 3), zero_weights.transpose(1, 3, 0, 2),
        control, unet_skips, norm_gains, norm_shifts,
    )


def solution(mesh):
    placed = (
        P("batch", "rows", None, None),
        P(None, "batch", "rows", None, None),
        P(),
        P(),
        P(None, None, None, None, "batch"),
        P(None, None, None, "batch"),
    )
    return jax.shard_map(
        on_device,
        mesh=mesh,
        in_specs=placed,
        out_specs=P(None, "batch", "rows", None, None),
        check_vma=False,
    )
```
